32 devices in a mesh: section: 2 (over core), dp: 16 (over z, y, x).
Axes of the slice: x: 2, y: 2, z: 4, core: 2. Of those that a mesh axis runs over, the one named last changes fastest.
Arguments:
- replay: bfloat16 [2048, 4096], P('dp'), may hold values from -6 to 6
- state_ids: int32 [2048], P('dp'), may hold values from 0 to 2047, as said below
- sampled: int32 [2048, 20], P('dp'), may hold values from 0 to 255
- targets: int32 [2048], P('dp'), may hold values from 0 to 19
- action_table: bfloat16 [256, 4096], replicated, may hold values from -6 to 6
- norm_gain: float32 [2, 4096], P('section'), may hold values from 0.5 to 1.5
- w_up: bfloat16 [2, 4096, 512], P('section', 'dp'), may hold values from -0.09375 to 0.09375
- w_down: bfloat16 [2, 512, 4096], P('section', 'dp'), may hold values from -0.25 to 0.25
Outputs:
- grad_up: float32 [2, 4096, 512], P('section', 'dp')
- grad_down: float32 [2, 512, 4096], P('section', 'dp')
- grad_gain: float32 [2, 4096], P('section')
- loss: float32 [], replicated
The draws below stay inside these ranges and needn't reach their ends.
Inputs may be any that keep to these rules, and one draw needn't show every extreme that they name: state_ids[i] // 128 == i // 128: a state's replay row lies in the same aligned block of 128 rows as the state.
All inputs are finite; a program needn't handle non-finite values.
Results may differ from the reference program's by a relative error of at most 0.011.
Values may be sent and summed in bfloat16 or wider, within the bound.
A program may use at most 128 MiB of HBM per device.

```python
import math
import jax
import jax.numpy as jnp
from jax import lax

D = 4096
FF = 512
VOCAB = 256
SAMPLES = 20
ROWS_DEV = 128
ROWS = 2048
N_LAYERS = 2


def draw_state_ids(key, part):
    offset = jnp.arange(ROWS) // ROWS_DEV * ROWS_DEV
    return (jax.random.randint(key, (ROWS,), 0, ROWS_DEV) + offset).astype(jnp.int32)


def with_ends(entries, key, low, top_value):
    longest = entries.shape.index(max(entries.shape))
    spots = []
    for shift in (0, 1):
        where = [jax.random.randint(jax.random.fold_in(key, axis), (), 0, length) for axis, length in enumerate(entries.shape)]
        where[longest] = (where[longest] + shift) % entries.shape[longest]
        spots.append(tuple(where))
    return entries.at[spots[0]].set(low).at[spots[1]].set(top_value)


def steps_of(rng, shape, cuts, low, high):
    loudness = 1.0
    for dim, blocks in cuts:
        heights = jax.random.uniform(jax.random.fold_in(jax.random.fold_in(rng, 6), dim), (blocks,), jnp.float32, low / len(cuts), high / len(cuts))
        loudness = loudness * jnp.repeat(jnp.exp(heights), shape[dim] // blocks).reshape((-1,) + (1,) * (len(shape) - 1 - dim))
    return loudness


def bell_draw(rng, dims, deviation, limit, shards=(), kind=jnp.bfloat16):
    values = deviation * jax.random.normal(rng, dims, jnp.float32)
    if shards:
        values = values * steps_of(rng, dims, shards, -0.22, 0.18)
    return jnp.clip(values, -limit, limit).astype(kind)


def setup_inputs(seed: int = 0) -> dict:
    arg_keys = jax.random.split(jax.random.key(seed), 9)
    return {
        "replay": bell_draw(arg_keys[0], (ROWS, D), 1.0, 6.0, ((0, 16),)),
        "state_ids": draw_state_ids(jax.random.fold_in(arg_keys[8], 71), 0),
        "sampled": with_ends(jax.random.randint(arg_keys[2], (ROWS, SAMPLES), 0, VOCAB), jax.random.fold_in(arg_keys[2], 1), 0, VOCAB - 1).astype(jnp.int32),
        "targets": with_ends(jax.random.randint(arg_keys[3], (ROWS,), 0, SAMPLES), jax.random.fold_in(arg_keys[3], 1), 0, SAMPLES - 1).astype(jnp.int32),
        "action_table": bell_draw(arg_keys[4], (VOCAB, D), 1.0, 6.0),
        "norm_gain": jnp.clip(1.0 + 0.1 * jax.random.normal(arg_keys[5], (N_LAYERS, D), jnp.float32), 0.5, 1.5),
        "w_up": bell_draw(arg_keys[6], (N_LAYERS, D, FF), D ** -0.5, 0.09375, ((0, 2), (1, 16))),
        "w_down": bell_draw(arg_keys[7], (N_LAYERS, FF, D), FF ** -0.5, 0.25, ((0, 2), (1, 16))),
    }


epsilon = 1e-06
logit_cap = 15.0

def contract_last(left, right):
    return lax.dot_general(left, right, (((1,), (1,)), ((), ())), preferred_element_type=jnp.float32)

def contract_first(left, right):
    return lax.dot_general(left, right, (((0,), (0,)), ((), ())), preferred_element_type=jnp.float32)

def layer_forward(states, gain_row, up_proj, down_proj):
    wide = states.astype(jnp.float32)
    recip = lax.rsqrt(lax.optimization_barrier(jnp.mean(wide * wide, -1, keepdims=True)) + epsilon)
    normed = (wide * recip * gain_row).astype(jnp.bfloat16)
    upper = jnp.dot(normed, up_proj, preferred_element_type=jnp.float32)
    sigm = jax.nn.sigmoid(upper)
    active = (upper * sigm).astype(jnp.bfloat16)
    result = (wide + jnp.dot(active, down_proj, preferred_element_type=jnp.float32)).astype(jnp.bfloat16)
    return (result, (wide, recip, normed, upper, sigm, active))

def layer_backward(grad_out, cache, gain_row, up_proj, down_proj):
    wide, recip, normed, upper, sigm, active = cache
    grad_act = contract_last(grad_out, down_proj)
    grad_upper = (grad_act * sigm * (1.0 + upper * (1.0 - sigm))).astype(jnp.bfloat16)
    grad_norm = contract_last(grad_upper, up_proj)
    scaled = grad_norm * gain_row
    gain_term = lax.optimization_barrier(jnp.sum(grad_norm * wide * recip, 0))
    grad_in = grad_out.astype(jnp.float32) + scaled * recip - wide * recip ** 3 * lax.optimization_barrier(jnp.mean(scaled * wide, -1, keepdims=True))
    return (grad_in.astype(jnp.bfloat16), grad_upper, gain_term)

def head_tail(chosen, targets, scale):
    bent = jnp.tanh(chosen / logit_cap)
    logits = logit_cap * bent
    expo = jnp.exp(logits)
    summed = lax.optimization_barrier(jnp.sum(expo, -1, keepdims=True))
    target_hot = (targets[:, None] == jnp.arange(chosen.shape[1])[None, :]).astype(jnp.float32)
    cross = jnp.log(summed[:, 0]) - lax.optimization_barrier(jnp.sum(logits * target_hot, -1))
    loss_sum = jnp.sum(cross) / ROWS_DEV
    d_logits = (expo / summed - target_hot) / ROWS_DEV
    d_chosen = d_logits * (1.0 - bent * bent) / scale
    return (loss_sum, d_chosen)

def reference(replay, state_ids, sampled, targets, action_table, norm_gain, w_up, w_down):
    picked = jnp.take(replay, state_ids, axis=0)
    embedded = jnp.take(action_table, sampled[:, 0], axis=0)
    hidden = (picked.astype(jnp.float32) + embedded.astype(jnp.float32)).astype(jnp.bfloat16)
    kept_inputs = []
    for layer_idx in range(N_LAYERS):
        kept_inputs.append(hidden)
        hidden, _ = layer_forward(hidden, norm_gain[layer_idx], w_up[layer_idx], w_down[layer_idx])
    scale = math.sqrt(D)
    scores = contract_last(hidden, action_table) / scale
    chosen = jnp.take_along_axis(scores, sampled, axis=1)
    loss_sum, d_chosen = head_tail(chosen, targets, scale)
    row_ids = jnp.arange(scores.shape[0])[:, None]
    d_scores = jnp.zeros(scores.shape, jnp.float32).at[row_ids, sampled].add(d_chosen)
    grad_state = jnp.dot(d_scores.astype(jnp.bfloat16), action_table, preferred_element_type=jnp.float32).astype(jnp.bfloat16)
    ups, downs, gains = ([], [], [])
    for layer_idx in reversed(range(N_LAYERS)):
        _, cache = layer_forward(kept_inputs[layer_idx], norm_gain[layer_idx], w_up[layer_idx], w_down[layer_idx])
        downs.append(contract_first(cache[5], grad_state))
        grad_state_new, grad_upper, gain_term = layer_backward(grad_state, cache, norm_gain[layer_idx], w_up[layer_idx], w_down[layer_idx])
        ups.append(contract_first(cache[2], grad_upper))
        gains.append(gain_term)
        grad_state = grad_state_new
    return (jnp.stack(ups[::-1]), jnp.stack(downs[::-1]), jnp.stack(gains[::-1]), loss_sum)
```

```python
import functools
import math

import jax
import jax.numpy as jnp
from jax import lax
from jax.experimental import pallas as pl
from jax.experimental.pallas import tpu as pltpu
from jax.sharding import PartitionSpec as P

ROWS_DEV = 128
epsilon = 1e-06
logit_cap = 15.0
bf16 = jnp.bfloat16
f32 = jnp.float32
i32 = jnp.int32


def contract_last(left, right):
    return lax.dot_general(left, right, (((1,), (1,)), ((), ())), preferred_element_type=f32)


def contract_first(left, right):
    return lax.dot_general(left, right, (((0,), (0,)), ((), ())), preferred_element_type=f32)


def dot(left, right):
    return jnp.dot(left, right, preferred_element_type=f32)


def spread(rows, column, axis):
    here = lax.broadcasted_iota(i32, (rows, rows), 0)
    there = lax.broadcasted_iota(i32, (rows, rows), 1)
    wide = jnp.broadcast_to(column, (rows, rows))
    return jnp.sum(jnp.where(here == there, wide, 0.0), axis, keepdims=True)


def local(source, dest, sem):
    made = pltpu.make_async_copy(source, dest, sem)
    made.start()
    return made


def arrive(dest, sem):
    pltpu.make_async_copy(dest, dest, sem).wait()


def push(source, dest, sems, dp, section):
    made = pltpu.make_async_remote_copy(
        src_ref=source,
        dst_ref=dest,
        send_sem=sems[0],
        recv_sem=sems[1],
        device_id={"dp": dp, "section": section},
        device_id_type=pl.DeviceIdType.MESH,
    )
    made.start()
    return made


class Dims:
    def __init__(self, sections, devices, held, width, ff, vocab, samples, up_held, ff_held):
        self.sections, self.devices, self.held, self.width = sections, devices, held, width
        self.ff, self.vocab, self.samples = ff, vocab, samples
        self.up_held, self.ff_held = up_held, ff_held
        self.outer = 2 * sections
        self.inner = devices // self.outer
        self.cut = width // self.outer
        self.group = 2 * held
        self.part = self.group // sections


def scratch_of(d):
    S, O, I, E = d.sections, d.outer, d.inner, 2 * d.sections + 1
    V, D = pltpu.VMEM, pltpu.SemaphoreType.DMA
    part, cut, ff, held = d.part, d.cut, d.ff, d.held
    return dict(
        rep=V((2, held, cut), bf16),
        tab=V((2, d.vocab, cut), bf16),
        gains=V((S, 1, cut), f32),
        ups=V((S, I, d.up_held, ff), bf16),
        downs=V((S, O, I, d.ff_held, cut), bf16),
        away=V((held, cut), bf16),
        states=V((S + 1, d.group, cut), bf16),
        ready=V((S, d.group, cut), bf16),
        picks=V((2, held, d.samples), i32),
        marks=V((2, held, 1), i32),
        mine_marks=V((held, 1), i32),
        counts=V((part, d.vocab), f32),
        hots=V((part, d.vocab), f32),
        acc=V((S, part, ff), f32),
        cuts=V((2 * S, S, part, ff), bf16),
        got=V((2 * S, S, part, ff), bf16),
        swap=V((2 * S, 2, part, ff), bf16),
        score_cuts=V((S, part, d.vocab), f32),
        score_got=V((S, part, d.vocab), f32),
        score_swap=V((2, part, d.vocab), f32),
        stat_cuts=V((S, S, 1, part), f32),
        stat_got=V((S, S, 1, part), f32),
        stat_swap=V((S, 2, 1, part), f32),
        uppers=V((S, part, ff), f32),
        recips=V((S, part, 1), f32),
        actives=V((S, S, part, ff), bf16),
        d_all=V((S, part, d.vocab), bf16),
        d_uppers=V((S, S, part, ff), bf16),
        pulls=V((S, S, 1, part), f32),
        grad=V((d.group, cut), bf16),
        g_up=V((S, I, d.up_held, ff), bf16),
        g_down=V((S, O, I, d.ff_held, cut), bf16),
        up_in=V((S, I - 1, d.up_held, ff), bf16),
        down_in=V((S, I - 1, O, d.ff_held, cut), bf16),
        up_sum=V((S, d.up_held, ff), bf16),
        down_sum=V((S, O, d.ff_held, cut), bf16),
        up_end=V((S, d.up_held, ff), bf16),
        down_end=V((S, O, d.ff_held, cut), bf16),
        small=V((S, 1, cut + 128), f32),
        small_in=V((S, I - 1, 1, cut + 128), f32),
        small_sum=V((S, 1, cut + 128), f32),
        small_end=V((S, O, 1, cut + 128), f32),
        load_sems=D((4,)),
        gain_sems=D((2, S)),
        start_sems=D((3, 2)),
        col_up=D((2, S)),
        col_down=D((2, S, O)),
        send_down=D((O, S)),
        square=D((2, 2, S, I)),
        trade=D((2, E, 3, S)),
        stats=D((2, E, 3, S)),
        fold=D((2, 3, S, I)),
        end_up=D((2, S)),
        end_down=D((2, O, S)),
        end_small=D((2, O, S)),
    )


def step_kernel(d, names, *refs):
    ins, outs, held_refs = refs[:8], refs[8:12], refs[12:]
    replay, table, ids, sampled, targets, gain, up, down = ins
    grad_up, grad_down, grad_gain, loss = outs
    m = dict(zip(names, held_refs))
    S, O, I, W, R, FF, V = d.sections, d.outer, d.inner, d.cut, d.held, d.ff, d.vocab
    GS, G = d.part, d.group
    scale = math.sqrt(d.width)
    c = lax.axis_index("section")
    pos = lax.axis_index("dp")
    z, j = lax.div(pos, I), lax.rem(pos, I)
    zh, p = lax.div(z, 2), lax.rem(z, 2)
    q = 2 * c + p
    partner = (z + 1 - 2 * p) * I + j
    ups, downs, states, ready = m["ups"], m["downs"], m["states"], m["ready"]
    pending = []

    def column(k):
        return lax.rem(z + k, O) * I + j

    def section(k):
        return lax.rem(c + k, S)

    def square(k):
        return lax.rem(j + k, I)

    def pair(name, *at):
        return m[name].at[(0, *at)], m[name].at[(1, *at)]

    def send(source, dest, sems, dp, to):
        made = push(source, dest, sems, dp, to)
        pending.append(made.wait_send)
        return made

    def deliver(mine, source, dest, sems, dp, to):
        @pl.when(mine)
        def _():
            local(source, dest, sems[1])

        @pl.when(jnp.logical_not(mine))
        def _():
            push(source, dest, sems, dp, to)

        def finish():
            @pl.when(jnp.logical_not(mine))
            def _():
                arrive(source, sems[0])

        pending.append(finish)

    def cut_of(n):
        return pl.ds(pl.multiple_of(n * W, W), W)

    other = 2 * c + 1 - p
    loads = []
    for n, at in ((0, other), (1, q)):
        loads.append(local(replay.at[:, cut_of(at)], m["rep"].at[n], m["load_sems"].at[n]))
        loads.append(local(table.at[:, cut_of(at)], m["tab"].at[n], m["load_sems"].at[2 + n]))

    barrier = pltpu.get_barrier_semaphore()
    peers = [(column(a), section(b)) for a in range(O) for b in range(S) if a or b]
    peers += [(z * I + square(k), c) for k in range(1, I)]
    for dp, to in peers:
        pl.semaphore_signal(
            barrier, inc=1, device_id={"dp": dp, "section": to}, device_id_type=pl.DeviceIdType.MESH
        )
    pl.semaphore_wait(barrier, len(peers))

    for k in range(S):
        home = (2 * lax.rem(zh + k, S) + p) * I + j
        sems = (m["col_up"].at[0, k], m["col_up"].at[1, c])
        if k == 0:
            deliver(c == zh, up, ups.at[c, j], sems, home, zh)
        else:
            send(up, ups.at[c, j], sems, home, zh)
    for a in range(O):
        for b in range(S):
            there = lax.rem(z + a, O)
            piece = down.at[:, cut_of(2 * section(b) + lax.rem(there, 2))]
            dest = downs.at[c, z, j]
            if a or b:
                sems = (m["send_down"].at[a, b], m["col_down"].at[1, c, a])
                send(piece, dest, sems, column(a), section(b))
            else:
                local(piece, dest, m["col_down"].at[1, c, 0])
    for k in range(1, S):
        sems = pair("gain_sems", k)
        send(gain.at[:, cut_of(2 * section(k) + p)], m["gains"].at[c], sems, pos, section(k))
    local(gain.at[:, cut_of(q)], m["gains"].at[c], m["gain_sems"].at[1, 0])

    m["mine_marks"][...] = spread(R, targets[...].astype(f32), 1).astype(i32)
    m["marks"][p] = m["mine_marks"][...]
    m["picks"][p] = sampled[...]
    extra = [
        send(sampled, m["picks"].at[p], (m["start_sems"].at[0, 0], m["start_sems"].at[0, 1]), partner, c),
        send(m["mine_marks"], m["marks"].at[p], (m["start_sems"].at[1, 0], m["start_sems"].at[1, 1]), partner, c),
    ]
    id_hot = (lax.broadcasted_iota(i32, (R, R), 0) == ids[...] - pos * R).astype(bf16)
    taken = (lax.broadcasted_iota(i32, (R, V), 1) == sampled[:, 0:1]).astype(bf16)
    for n in range(2):
        loads[2 * n].wait()
        loads[2 * n + 1].wait()
        start = (contract_first(id_hot, m["rep"][n]) + dot(taken, m["tab"][n])).astype(bf16)
        mine_rows = pl.ds(pl.multiple_of(p * R, R), R)
        if n == 0:
            m["away"][...] = start
            sems = (m["start_sems"].at[2, 0], m["start_sems"].at[2, 1])
            moved = send(m["away"], states.at[0, mine_rows], sems, partner, c)
        else:
            states[0, mine_rows] = start

    for got in extra:
        got.wait_recv()
    first_row = c * GS
    chip, row = lax.div(first_row, R), pl.multiple_of(lax.rem(first_row, R), GS)
    picks = m["picks"][chip, pl.ds(row, GS)]
    marks = m["marks"][chip, pl.ds(row, GS)]
    actions = lax.broadcasted_iota(i32, (GS, V), 1)
    counts, hots = jnp.zeros((GS, V), f32), jnp.zeros((GS, V), f32)
    for k in range(d.samples):
        hit = jnp.where(picks[:, k : k + 1] == actions, 1.0, 0.0)
        counts += hit
        hots += jnp.where(marks == k, hit, 0.0)
    m["counts"][...] = counts
    m["hots"][...] = hots

    fans = {}

    def fan_up(layer):
        arrive(ups.at[layer, j], m["col_up"].at[1, layer])
        fans[0, layer] = [
            send(ups.at[layer, j], ups.at[layer, j], pair("square", 0, layer, k), z * I + square(k), c)
            for k in range(1, I)
        ]

    def fan_down(layer):
        for a in range(O):
            giver = lax.rem(z + O - a, O)
            arrive(downs.at[layer, giver, j], m["col_down"].at[1, layer, a])
        mine = downs.at[layer, :, j]
        fans[1, layer] = [
            send(mine, mine, pair("square", 1, layer, k), z * I + square(k), c) for k in range(1, I)
        ]

    def land(made):
        for copy in made:
            copy.wait_recv()

    def trade(e, partial, cuts, got, swap, stat=None, slot=None):
        m_acc = m["acc"]
        span = partial.shape[1]
        split = partial.reshape(S, GS, span)
        m_acc[:, :, :span] = split
        cuts[...] = split.astype(cuts.dtype)
        sent = [
            send(cuts.at[section(k)], got.at[k], pair("trade", e, 0, k), pos, section(k))
            for k in range(1, S)
        ]
        rows = []
        if stat is not None:
            for k in range(S):
                m["stat_cuts"][slot, k] = spread(GS, stat[k * GS : (k + 1) * GS], 0)
            rows = [
                send(
                    m["stat_cuts"].at[slot, section(k)],
                    m["stat_got"].at[slot, k],
                    pair("stats", e, 0, k),
                    pos,
                    section(k),
                )
                for k in range(1, S)
            ]

        def finish():
            land(sent)
            total = m_acc[c, :, :span]
            for k in range(1, S):
                total += got[k].astype(f32)
            swap[0] = total.astype(swap.dtype)
            over = send(swap.at[0], swap.at[1], pair("trade", e, 1, 0), partner, c)
            if stat is not None:
                land(rows)
                square_sum = m["stat_cuts"][slot, c]
                for k in range(1, S):
                    square_sum += m["stat_got"][slot, k]
                m["stat_swap"][slot, 0] = square_sum
                over_row = send(
                    m["stat_swap"].at[slot, 0],
                    m["stat_swap"].at[slot, 1],
                    pair("stats", e, 1, 0),
                    partner,
                    c,
                )

            def end():
                squares = None
                if stat is not None:
                    over_row.wait_recv()
                    squares = spread(GS, square_sum + m["stat_swap"][slot, 1], 1)
                over.wait_recv()
                return total + swap[1].astype(f32), squares

            return end

        return finish

    def gather(e, held):
        return [
            send(held.at[c], held.at[c], pair("trade", e, 2, k), pos, section(k))
            for k in range(1, S)
        ]

    for layer in range(S):
        fan_up(layer)
        fan_down(layer)
    moved.wait_recv()
    arrive(m["gains"].at[c], m["gain_sems"].at[1, 0])
    for k in range(1, S):
        giver = lax.rem(c + S - k, S)
        arrive(m["gains"].at[giver], m["gain_sems"].at[1, k])

    def ups_of(layer):
        return ups[layer].reshape(W, FF)

    def downs_of(layer):
        return downs[layer].reshape(FF, W)

    for layer in range(S):
        wide = states[layer].astype(f32)
        ready[layer] = (wide * m["gains"][layer]).astype(bf16)
        stat = jnp.sum(wide * wide, -1, keepdims=True)
        land(fans[0, layer])
        partial = dot(ready[layer], ups_of(layer))
        middle = trade(layer, partial, m["cuts"].at[layer], m["got"].at[layer], m["swap"].at[layer], stat, layer)
        total, squares = middle()()
        factor = lax.rsqrt(squares / d.width + epsilon)
        value = total * factor
        m["uppers"][layer] = value
        m["recips"][layer] = factor
        held = m["actives"].at[layer]
        held[c] = (value * jax.nn.sigmoid(value)).astype(bf16)
        moving = gather(layer, held)
        land(fans[1, layer])
        land(moving)
        states[layer + 1] = (
            states[layer].astype(f32) + dot(m["actives"][layer].reshape(G, FF), downs_of(layer))
        ).astype(bf16)

    part = contract_last(states[S], m["tab"][1])
    total, _ = trade(S, part, m["score_cuts"], m["score_got"], m["score_swap"])()()
    bent = jnp.tanh(total / scale / logit_cap)
    logits = logit_cap * bent
    counts, hots = m["counts"][...], m["hots"][...]
    weighted = counts * jnp.exp(logits)
    summed = jnp.sum(weighted, -1, keepdims=True)
    d_scores = (weighted / summed - hots) / ROWS_DEV * (1.0 - bent * bent) / scale
    m["d_all"][c] = d_scores.astype(bf16)
    moving = gather(S, m["d_all"])
    cross = jnp.log(summed) - jnp.sum(logits * hots, -1, keepdims=True)
    counted = jnp.where(p == 0, 1.0 / ROWS_DEV, 0.0)
    loss_here = jnp.broadcast_to(jnp.sum(cross, 0, keepdims=True) * counted, (1, 128))
    land(moving)
    m["grad"][...] = dot(m["d_all"][...].reshape(G, V), m["tab"][1]).astype(bf16)

    folds = {}

    def fold(kind, layer, source, dest):
        folds[kind, layer] = [
            send(source(square(k)), dest.at[layer, k - 1], pair("fold", kind, layer, k), z * I + square(k), c)
            for k in range(1, I)
        ]

    for layer in reversed(range(S)):
        e = S + 1 + layer
        slot = S + layer
        grad = m["grad"][...]
        part = contract_last(grad, downs_of(layer))
        middle = trade(e, part, m["cuts"].at[slot], m["got"].at[slot], m["swap"].at[slot])
        actives = m["actives"][layer].reshape(G, FF)
        end = middle()
        m["g_down"][layer] = contract_first(actives, grad).astype(bf16).reshape(O, I, d.ff_held, W)
        fold(1, layer, lambda at: m["g_down"].at[layer, :, at], m["down_in"])
        total, _ = end()
        value, factor = m["uppers"][layer], m["recips"][layer]
        sigm = jax.nn.sigmoid(value)
        d_upper = (total * sigm * (1.0 + value * (1.0 - sigm)) * factor).astype(bf16)
        held = m["d_uppers"].at[layer]
        held[c] = d_upper
        moving = gather(e, held)
        if layer:
            pull = jnp.sum(d_upper.astype(f32) * value, -1, keepdims=True) * factor / d.width
            m["pulls"][layer, c] = spread(GS, pull, 0)
            moving += [
                send(
                    m["pulls"].at[layer, c],
                    m["pulls"].at[layer, c],
                    pair("stats", e, 2, k),
                    pos,
                    section(k),
                )
                for k in range(1, S)
            ]
        land(moving)
        d_all = m["d_uppers"][layer].reshape(G, FF)
        wide = states[layer].astype(f32)
        d_normed = contract_last(d_all, ups_of(layer))
        m["small"][layer, :, :W] = jnp.sum(d_normed * wide, 0, keepdims=True)
        m["small"][layer, :, W:] = loss_here
        fold(2, layer, lambda at: m["small"].at[layer], m["small_in"])
        if layer:
            columns = jnp.concatenate([spread(GS, m["pulls"][layer, k], 1) for k in range(S)], 0)
            m["grad"][...] = (
                grad.astype(f32) + d_normed * m["gains"][layer] - wide * columns
            ).astype(bf16)
        m["g_up"][layer] = contract_first(ready[layer], d_all).astype(bf16).reshape(I, d.up_held, FF)
        fold(0, layer, lambda at: m["g_up"].at[layer, at], m["up_in"])

    home = q * I + j
    for layer in reversed(range(S)):
        land(folds[1, layer])
        value = m["g_down"][layer, :, j].astype(f32)
        for k in range(1, I):
            value += m["down_in"][layer, k - 1].astype(f32)
        m["down_sum"][layer] = value.astype(bf16)
        for a in range(O):
            there = lax.rem(z + a, O)
            source, dest = m["down_sum"].at[layer, there], m["down_end"].at[zh, q]
            sems = (m["end_down"].at[0, a, layer], m["end_down"].at[1, a, c])
            if a:
                send(source, dest, sems, column(a), layer)
            else:
                deliver(c == layer, source, dest, sems, pos, layer)
        land(folds[2, layer])
        value = m["small"][layer]
        for k in range(1, I):
            value += m["small_in"][layer, k - 1]
        m["small_sum"][layer] = value
        for a in range(O):
            source, dest = m["small_sum"].at[layer], m["small_end"].at[zh, q]
            sems = (m["end_small"].at[0, a, layer], m["end_small"].at[1, a, c])
            if a:
                send(source, dest, sems, column(a), layer)
            else:
                deliver(c == layer, source, dest, sems, pos, layer)
        land(folds[0, layer])
        value = m["g_up"][layer, j].astype(f32)
        for k in range(1, I):
            value += m["up_in"][layer, k - 1].astype(f32)
        m["up_sum"][layer] = value.astype(bf16)
        sems = (m["end_up"].at[0, layer], m["end_up"].at[1, zh])
        mine = jnp.logical_and(c == zh, c == layer)
        deliver(mine, m["up_sum"].at[layer], m["up_end"].at[zh], sems, home, layer)

    for a in range(O):
        giver = lax.rem(z + O - a, O)
        for b in range(S):
            cut = 2 * b + lax.rem(giver, 2)
            arrive(m["down_end"].at[lax.div(giver, 2), cut], m["end_down"].at[1, a, b])
            arrive(m["small_end"].at[lax.div(giver, 2), cut], m["end_small"].at[1, a, b])
    lost = jnp.zeros((1, 128), f32)
    for cut in range(O):
        value = jnp.zeros((d.ff_held, W), f32)
        row = jnp.zeros((1, W), f32)
        for h in range(S):
            value += m["down_end"][h, cut].astype(f32)
            row += m["small_end"][h, cut, :, :W]
            lost += m["small_end"][h, cut, :, W:]
        grad_down[:, cut * W : (cut + 1) * W] = value
        grad_gain[:, cut * W : (cut + 1) * W] = row
    loss[...] = lost
    value = jnp.zeros((d.up_held, FF), f32)
    for h in range(S):
        arrive(m["up_end"].at[h], m["end_up"].at[1, h])
        value += m["up_end"][h].astype(f32)
    grad_up[...] = value
    for finish in pending:
        finish()


def on_device(replay, state_ids, sampled, targets, action_table, norm_gain, w_up, w_down):
    held, width = replay.shape
    d = Dims(
        lax.axis_size("section"),
        lax.axis_size("dp"),
        held,
        width,
        w_up.shape[2],
        action_table.shape[0],
        sampled.shape[1],
        w_up.shape[1],
        w_down.shape[1],
    )
    scratch = scratch_of(d)
    vmem = pl.BlockSpec(memory_space=pltpu.VMEM)
    hbm = pl.BlockSpec(memory_space=pl.ANY)
    outs = ((d.up_held, d.ff), (d.ff_held, width), (1, width), (1, 128))
    grad_up, grad_down, grad_gain, loss = pl.pallas_call(
        functools.partial(step_kernel, d, tuple(scratch)),
        out_shape=[jax.ShapeDtypeStruct(shape, f32) for shape in outs],
        in_specs=[hbm, hbm, vmem, vmem, vmem, vmem, vmem, vmem],
        out_specs=[vmem] * 4,
        scratch_shapes=list(scratch.values()),
        compiler_params=pltpu.CompilerParams(
            collective_id=0, has_side_effects=True, vmem_limit_bytes=60 * 1024 * 1024
        ),
    )(
        replay,
        action_table,
        state_ids[None, :],
        sampled,
        targets[None, :],
        norm_gain,
        w_up[0],
        w_down[0],
    )
    return (grad_up[None], grad_down[None], grad_gain, loss[0, 0])


def solution(mesh):
    return jax.shard_map(
        on_device,
        mesh=mesh,
        in_specs=(
            P("dp", None),
            P("dp"),
            P("dp", None),
            P("dp"),
            P(),
            P("section", None),
            P("section", "dp", None),
            P("section", "dp", None),
        ),
        out_specs=(P("section", "dp", None), P("section", "dp", None), P("section", None), P()),
        check_vma=False,
    )
```

```python
import functools
import math
import types

import jax
import jax.numpy as jnp
from jax import lax
from jax.experimental import pallas as pl
from jax.experimental.pallas import tpu as pltpu
from jax.sharding import PartitionSpec as P

ROWS_DEV = 128
epsilon = 1e-06
logit_cap = 15.0
bf16 = jnp.bfloat16
f32 = jnp.float32
i32 = jnp.int32
DP, SECTION = "dp", "section"


def contract_last(left, right):
    return lax.dot_general(left, right, (((1,), (1,)), ((), ())), preferred_element_type=f32)


def contract_first(left, right):
    return lax.dot_general(left, right, (((0,), (0,)), ((), ())), preferred_element_type=f32)


def dot(left, right):
    return jnp.dot(left, right, preferred_element_type=f32)


def spread(rows, column, axis):
    here = lax.broadcasted_iota(i32, (rows, rows), 0)
    there = lax.broadcasted_iota(i32, (rows, rows), 1)
    wide = jnp.broadcast_to(column, (rows, rows))
    return jnp.sum(jnp.where(here == there, wide, 0.0), axis, keepdims=True)


def local(source, dest, sem):
    made = pltpu.make_async_copy(source, dest, sem)
    made.start()
    return made


def arrive(dest, sem):
    pltpu.make_async_copy(dest, dest, sem).wait()


def flip(j, k):
    low, high = lax.rem(j, 2), lax.div(j, 2)
    return (2 * (1 - high) if k & 2 else 2 * high) + ((1 - low) if k & 1 else low)


def push(source, dest, sems, dp, section):
    made = pltpu.make_async_remote_copy(
        src_ref=source,
        dst_ref=dest,
        send_sem=sems[0],
        recv_sem=sems[1],
        device_id={DP: dp, SECTION: section},
        device_id_type=pl.DeviceIdType.MESH,
    )
    made.start()
    return made


class Dims:
    def __init__(self, sections, devices, held, width, ff, vocab, samples, up_held, ff_held):
        self.sections, self.devices, self.held, self.width = sections, devices, held, width
        self.ff, self.vocab, self.samples = ff, vocab, samples
        self.up_held, self.ff_held = up_held, ff_held
        self.outer = 2 * sections
        self.inner = devices // self.outer
        self.cut = width // self.outer
        self.group = 2 * held
        self.part = self.group // sections
        self.factored = self.inner == 4 and self.up_held % 128 == 0


def scratch_of(d):
    S, O, I, E = d.sections, d.outer, d.inner, 2 * d.sections + 1
    V, D = pltpu.VMEM, pltpu.SemaphoreType.DMA
    part, cut, ff, held, others = d.part, d.cut, d.ff, d.held, max(S - 1, 1)
    if d.factored:
        kinds = dict(
            others=V((S, I, d.group, d.up_held), bf16),
            down_in=V((S, 6, O // 2, d.ff_held, cut), bf16),
            down_part=V((S, 2, O // 2, d.ff_held, cut), bf16),
            d_uppers=V((S, I, S, part, ff), bf16),
            other_sems=D((2, S)),
            upper_send=D((S,)),
            upper_recv=D((S, I - 1)),
            share_sems=D((2, S)),
            half_send=D((S,)),
            half_recv=D((S, 3)),
        )
    else:
        kinds = dict(
            g_up=V((S, I, d.up_held, ff), bf16),
            up_in=V((S, I - 1, d.up_held, ff), bf16),
            down_in=V((S, I - 1, O, d.ff_held, cut), bf16),
            d_uppers=V((S, 1, S, part, ff), bf16),
            fold=D((2, 2, S, I - 1)),
        )
    return dict(
        **kinds,
        rep=V((2, held, cut), bf16),
        tab=V((2, d.vocab, cut), bf16),
        gains=V((S, 1, cut), f32),
        ups=V((S, I, d.up_held, ff), bf16),
        downs=V((S, O, I, d.ff_held, cut), bf16),
        away=V((held, cut), bf16),
        states=V((S + 1, d.group, cut), bf16),
        ready=V((S, d.group, cut), bf16),
        picks=V((2, d.samples, held), i32),
        marks=V((2, 1, held), i32),
        counts=V((held, d.vocab), f32),
        hots=V((held, d.vocab), f32),
        acc=V((S, part, ff), f32),
        cuts=V((2 * S, S, part, ff), bf16),
        got=V((2 * S, S, part, ff), bf16),
        swap=V((2 * S, 2, part, ff), bf16),
        score_cuts=V((S, part, d.vocab), f32),
        score_got=V((S, part, d.vocab), f32),
        score_swap=V((2, part, d.vocab), f32),
        stat_cuts=V((S, S, 1, part), f32),
        stat_got=V((S, S, 1, part), f32),
        stat_swap=V((S, 2, 1, part), f32),
        uppers=V((S, part, ff), f32),
        recips=V((S, part, 1), f32),
        actives=V((S, S, part, ff), bf16),
        d_all=V((S, part, d.vocab), bf16),
        pulls=V((S, S, 1, part), f32),
        grad=V((d.group, cut), bf16),
        g_down=V((S, O, I, d.ff_held, cut), bf16),
        up_sum=V((S, d.up_held, ff), bf16),
        down_sum=V((S, O, d.ff_held, cut), bf16),
        up_end=V((S, d.up_held, ff), bf16),
        down_end=V((S, O, d.ff_held, cut), bf16),
        small=V((S, 1, cut + 128), f32),
        small_in=V((S, I - 1, 1, cut + 128), f32),
        small_sum=V((S, 1, cut + 128), f32),
        small_end=V((S, O, 1, cut + 128), f32),
        load_sems=D((4,)),
        gain_sems=D((2, S)),
        start_sems=D((3, 2)),
        col_up=D((2, S)),
        col_down=D((S,)),
        send_down=D((2,)),
        square_send=D((2, S)),
        square_recv=D((2, S, I - 1)),
        trade=D((2, E, 3, others)),
        tallies=D((2, S, 2, others)),
        pull_sems=D((2, S, others)),
        small_fold=D((2, S)),
        end_up=D((S,)),
        end_up_recv=D((1,)),
        end_down=D((2, S)),
        end_down_recv=D((1,)),
        end_small=D((2, S)),
        end_small_recv=D((1,)),
    )


def step_kernel(d, names, *refs):
    ins, outs, held_refs = refs[:8], refs[8:12], refs[12:]
    replay, table, ids, sampled, targets, gain, up, down = ins
    grad_up, grad_down, grad_gain, loss = outs
    m = types.SimpleNamespace(**dict(zip(names, held_refs)))
    S, O, I, W, R, FF, V = d.sections, d.outer, d.inner, d.cut, d.held, d.ff, d.vocab
    GS, G = d.part, d.group
    scale = math.sqrt(d.width)
    c = lax.axis_index(SECTION)
    pos = lax.axis_index(DP)
    z, j = lax.div(pos, I), lax.rem(pos, I)
    zh, p = lax.div(z, 2), lax.rem(z, 2)
    q = 2 * c + p
    partner = (z + 1 - 2 * p) * I + j
    ups, downs, states, ready = m.ups, m.downs, m.states, m.ready
    pending = []

    def column(k):
        return lax.rem(z + k, O) * I + j

    def section(k):
        return lax.rem(c + k, S)

    def square(k):
        return lax.rem(j + k, I)

    def pair(held, *at):
        return held.at[(0, *at)], held.at[(1, *at)]

    def send(source, dest, sems, dp, to, track=True):
        made = push(source, dest, sems, dp, to)
        if track:
            pending.append(made.wait_send)
        return made

    def settle(span, sem):
        pending.append(lambda: arrive(span, sem))

    def deliver(mine, source, dest, sems, dp, to, track=True):
        @pl.when(mine)
        def _():
            local(source, dest, sems[1])

        @pl.when(jnp.logical_not(mine))
        def _():
            push(source, dest, sems, dp, to)

        def finish():
            @pl.when(jnp.logical_not(mine))
            def _():
                arrive(source, sems[0])

        if track:
            pending.append(finish)

    def cut_of(n):
        return pl.ds(pl.multiple_of(n * W, W), W)

    other = 2 * c + 1 - p
    loads = []
    for n, at in ((0, other), (1, q)):
        loads.append(local(replay.at[:, cut_of(at)], m.rep.at[n], m.load_sems.at[n]))
        loads.append(local(table.at[:, cut_of(at)], m.tab.at[n], m.load_sems.at[2 + n]))

    barrier = pltpu.get_barrier_semaphore()
    peers = [(column(a), section(b)) for a in range(O) for b in range(S) if a or b]
    peers += [(z * I + square(k), c) for k in range(1, I)]
    for dp, to in peers:
        pl.semaphore_signal(
            barrier, inc=1, device_id={DP: dp, SECTION: to}, device_id_type=pl.DeviceIdType.MESH
        )
    pl.semaphore_wait(barrier, len(peers))

    def up_column():
        for k in range(S):
            home = (2 * lax.rem(zh + k, S) + p) * I + j
            sems = (m.col_up.at[0, k], m.col_up.at[1, c])
            if k == 0:
                deliver(c == zh, up, ups.at[c, j], sems, home, zh, False)
            else:
                push(up, ups.at[c, j], sems, home, zh)

    def down_column():
        for a in range(O):
            for b in range(S):
                there = lax.rem(z + a, O)
                piece = down.at[:, cut_of(2 * section(b) + lax.rem(there, 2))]
                dest = downs.at[c, z, j]
                if a or b:
                    sems = (m.send_down.at[0 if a else 1], m.col_down.at[c])
                    push(piece, dest, sems, column(a), section(b))
                else:
                    local(piece, dest, m.col_down.at[c])

    def drain_columns():
        @pl.when(c != zh)
        def _():
            arrive(up, m.col_up.at[0, 0])

        for k in range(1, S):
            arrive(up, m.col_up.at[0, k])
        arrive(downs.at[:, pl.ds(0, O - 1), 0], m.send_down.at[0])
        if S > 1:
            arrive(downs.at[pl.ds(0, S - 1), 0, 0], m.send_down.at[1])

    first = c == 0
    later = c != 0
    extra = [
        send(sampled, m.picks.at[p], (m.start_sems.at[0, 0], m.start_sems.at[0, 1]), partner, c),
        send(targets, m.marks.at[p], (m.start_sems.at[1, 0], m.start_sems.at[1, 1]), partner, c),
    ]

    @pl.when(first)
    def _():
        up_column()
        down_column()

    for k in range(1, S):
        sems = pair(m.gain_sems, k)
        send(gain.at[:, cut_of(2 * section(k) + p)], m.gains.at[c], sems, pos, section(k))
    local(gain.at[:, cut_of(q)], m.gains.at[c], m.gain_sems.at[1, 0])

    id_hot = (lax.broadcasted_iota(i32, (R, R), 0) == ids[...] - pos * R).astype(bf16)
    taken = (lax.broadcasted_iota(i32, (V, R), 0) == sampled[0:1]).astype(bf16)
    for n in range(2):
        loads[2 * n].wait()
        loads[2 * n + 1].wait()
        start = (contract_first(id_hot, m.rep[n]) + contract_first(taken, m.tab[n])).astype(bf16)
        mine_rows = pl.ds(pl.multiple_of(p * R, R), R)
        if n == 0:
            m.away[...] = start
            sems = (m.start_sems.at[2, 0], m.start_sems.at[2, 1])
            moved = send(m.away, states.at[0, mine_rows], sems, partner, c)
        else:
            states[0, mine_rows] = start

    chip, row = lax.div(c * GS, R), pl.multiple_of(lax.rem(c * GS, R), GS)

    def count():
        m.marks[p] = targets[...]
        m.picks[p] = sampled[...]
        land(extra)
        picks, marks = m.picks[chip], m.marks[chip]
        actions = lax.broadcasted_iota(i32, (V, R), 0)
        counts, hots = jnp.zeros((V, R), f32), jnp.zeros((V, R), f32)
        for k in range(d.samples):
            hit = jnp.where(picks[k : k + 1] == actions, 1.0, 0.0)
            counts += hit
            hots += jnp.where(marks == k, hit, 0.0)
        m.counts[...] = counts.T
        m.hots[...] = hots.T

    fans = {}
    relayed = I == 4

    def block(kind, layer, at, half=None):
        if kind == 0:
            if half is None:
                return ups.at[layer, at]
            return ups.at[layer, at, pl.ds(half * (d.up_held // 2), d.up_held // 2)]
        if half is None:
            return downs.at[layer, :, at]
        return downs.at[layer, pl.ds(half * (O // 2), O // 2), at]

    def blocks(kind, layer, n):
        return ups.at[layer, pl.ds(0, n)] if kind == 0 else downs.at[layer, :, pl.ds(0, n)]

    def fan(kind, layer):
        if kind == 0:
            arrive(ups.at[layer, j], m.col_up.at[1, layer])
        else:
            arrive(downs.at[layer, :, j], m.col_down.at[layer])
        going, coming = m.square_send.at[kind, layer], m.square_recv.at[kind, layer]
        made = fans[kind, layer] = {}
        if relayed:
            for k, half, n in ((1, 0, 0), (2, 1, 1), (1, 1, 2), (2, 0, 2)):
                view = block(kind, layer, j, half)
                to = z * I + flip(j, k)
                made[n] = send(view, view, (going, coming.at[n]), to, c, False)
        else:
            view = block(kind, layer, j)
            for k in range(1, I):
                to = z * I + square(k)
                made[k] = send(view, view, (going, coming.at[k - 1]), to, c, False)
        settle(blocks(kind, layer, I - 1), going)

    def relay(kind, layer):
        if relayed:
            made = fans[kind, layer]
            going, coming = m.square_send.at[kind, layer], m.square_recv.at[kind, layer]
            for k, half in ((1, 0), (2, 1)):
                land([made[half]])
                view = block(kind, layer, flip(j, k), half)
                send(view, view, (going, coming.at[2]), z * I + flip(j, 3 - k), c, False)

    def land_fan(kind, layer):
        if relayed:
            arrive(blocks(kind, layer, 2), m.square_recv.at[kind, layer, 2])
        else:
            land(fans[kind, layer])

    def land(made):
        for copy in made.values() if isinstance(made, dict) else made:
            copy.wait_recv()

    def tally(e, slot, stat):
        for k in range(S):
            m.stat_cuts[slot, k] = spread(GS, stat[k * GS : (k + 1) * GS], 0)
        rows = [
            send(
                m.stat_cuts.at[slot, section(k)],
                m.stat_got.at[slot, k],
                pair(m.tallies, slot, 0, k - 1),
                pos,
                section(k),
            )
            for k in range(1, S)
        ]

        def finish():
            land(rows)
            row = m.stat_cuts[slot, c]
            for k in range(1, S):
                row += m.stat_got[slot, k]
            m.stat_swap[slot, 0] = row
            swap = m.stat_swap.at[slot]
            over = send(swap.at[0], swap.at[1], pair(m.tallies, slot, 1, 0), partner, c)

            def end():
                land([over])
                return spread(GS, row + m.stat_swap[slot, 1], 1)

            return end

        return finish

    def trade(e, partial, cuts, got, swap):
        m_acc = m.acc
        span = partial.shape[1]
        split = partial.reshape(S, GS, span)
        m_acc[:, :, :span] = split
        cuts[...] = split.astype(cuts.dtype)
        sent = [
            send(cuts.at[section(k)], got.at[k], pair(m.trade, e, 0, k - 1), pos, section(k))
            for k in range(1, S)
        ]

        def finish():
            land(sent)
            total = m_acc[c, :, :span]
            for k in range(1, S):
                total += got[k].astype(f32)
            swap[0] = total.astype(swap.dtype)
            over = send(swap.at[0], swap.at[1], pair(m.trade, e, 1, 0), partner, c)

            def end():
                land([over])
                return total + swap[1].astype(f32)

            return end

        return finish

    def gather(e, held):
        return [
            send(held.at[c], held.at[c], pair(m.trade, e, 2, k - 1), pos, section(k))
            for k in range(1, S)
        ]

    fan(0, 0)
    count()
    relay(0, 0)
    fan(1, 0)
    pl.when(later)(up_column)
    moved.wait_recv()
    arrive(m.gains.at[c], m.gain_sems.at[1, 0])
    for k in range(1, S):
        giver = lax.rem(c + S - k, S)
        arrive(m.gains.at[giver], m.gain_sems.at[1, k])

    def lend(layer):
        if d.factored:
            own = pl.ds(pl.multiple_of(j * d.up_held, 128), d.up_held)
            m.others[layer, j] = ready[layer, :, own]
            for k in (1, 2, 3):
                send(
                    ready.at[layer, :, pl.ds(pl.multiple_of(flip(j, k) * d.up_held, 128), d.up_held)],
                    m.others.at[layer, j],
                    pair(m.other_sems, layer),
                    z * I + flip(j, k),
                    c,
                    False,
                )
            settle(m.others.at[layer, pl.ds(0, I - 1)], m.other_sems.at[0, layer])

    def ups_of(layer):
        return ups[layer].reshape(W, FF)

    def downs_of(layer):
        return downs[layer].reshape(FF, W)

    for layer in range(S):
        wide = states[layer].astype(f32)
        ready[layer] = (wide * m.gains[layer]).astype(bf16)
        counted = tally(layer, layer, jnp.sum(wide * wide, -1, keepdims=True))
        land_fan(0, layer)
        partial = dot(ready[layer], ups_of(layer))
        middle = trade(layer, partial, m.cuts.at[layer], m.got.at[layer], m.swap.at[layer])
        counted = counted()
        if layer == 0:
            pl.when(later)(down_column)
        relay(1, layer)
        if layer + 1 == S:
            for held_layer in range(S):
                lend(held_layer)
        end = middle()
        if layer + 1 < S:
            fan(0, layer + 1)
        factor = lax.rsqrt(counted() / d.width + epsilon)
        value = end() * factor
        m.uppers[layer] = value
        m.recips[layer] = factor
        held = m.actives.at[layer]
        held[c] = (value * jax.nn.sigmoid(value)).astype(bf16)
        moving = gather(layer, held)
        if layer + 1 < S:
            relay(0, layer + 1)
            fan(1, layer + 1)
        land_fan(1, layer)
        land(moving)
        states[layer + 1] = (
            states[layer].astype(f32) + dot(m.actives[layer].reshape(G, FF), downs_of(layer))
        ).astype(bf16)

    part = contract_last(states[S], m.tab[1])
    total = trade(S, part, m.score_cuts, m.score_got, m.score_swap)()()
    bent = jnp.tanh(total / scale / logit_cap)
    logits = logit_cap * bent
    counts, hots = m.counts[pl.ds(row, GS)], m.hots[pl.ds(row, GS)]
    weighted = counts * jnp.exp(logits)
    summed = jnp.sum(weighted, -1, keepdims=True)
    d_scores = (weighted / summed - hots) / ROWS_DEV * (1.0 - bent * bent) / scale
    m.d_all[c] = d_scores.astype(bf16)
    moving = gather(S, m.d_all)
    cross = jnp.log(summed) - jnp.sum(logits * hots, -1, keepdims=True)
    counted = jnp.where(p == 0, 1.0 / ROWS_DEV, 0.0)
    loss_here = jnp.broadcast_to(jnp.sum(cross, 0, keepdims=True) * counted, (1, 128))
    land(moving)
    m.grad[...] = dot(m.d_all[...].reshape(G, V), m.tab[1]).astype(bf16)

    folds = {}

    def fold(kind, layer, source, dest):
        folds[kind, layer] = [
            send(source(square(k)), dest.at[layer, k - 1], pair(m.fold, kind, layer, k - 1), z * I + square(k), c)
            for k in range(1, I)
        ]

    def fold_down(layer):
        if not d.factored:
            fold(1, layer, lambda at: m.g_down.at[layer, :, at], m.down_in)
            return
        made = folds[1, layer] = {}
        for n, k, at, half in ((1, 1, 3, 0), (3, 2, 3, 1), (0, 1, 1, 0), (2, 2, 2, 1)):
            source = m.g_down.at[layer, pl.ds(half * (O // 2), O // 2), flip(j, at)]
            sems = (m.half_send.at[layer], m.half_recv.at[layer, {1: 0, 3: 1}.get(n, 2)])
            made[n] = send(source, m.down_in.at[layer, n], sems, z * I + flip(j, k), c, False)

    def refold_down(layer):
        if not d.factored:
            return
        made = folds[1, layer]
        for n, k, half in ((1, 2, 0), (3, 1, 1)):
            land([made[n]])
            own = m.g_down[layer, half * (O // 2) : (half + 1) * (O // 2), flip(j, k)]
            into = m.down_part.at[layer, half]
            into[...] = (own.astype(f32) + m.down_in[layer, n].astype(f32)).astype(bf16)
            sems = (m.half_send.at[layer], m.half_recv.at[layer, 2])
            send(into, m.down_in.at[layer, 4 + half], sems, z * I + flip(j, k), c, False)
        settle(m.down_in.at[layer], m.half_send.at[layer])

    def down_total(layer):
        if not d.factored:
            land(folds[1, layer])
            value = m.g_down[layer, :, j].astype(f32)
            for k in range(1, I):
                value += m.down_in[layer, k - 1].astype(f32)
            m.down_sum[layer] = value.astype(bf16)
            return
        arrive(m.down_in.at[layer, pl.ds(0, 4)], m.half_recv.at[layer, 2])
        for half in range(2):
            rows = pl.ds(half * (O // 2), O // 2)
            value = m.g_down[layer, rows, j].astype(f32)
            for n in (2 * half, 4 + half):
                value += m.down_in[layer, n].astype(f32)
            m.down_sum[layer, rows] = value.astype(bf16)

    def share(layer):
        held = m.d_uppers.at[layer, j, c]
        folds[0, layer] = [
            (k, send(held, held, (m.upper_send.at[layer], m.upper_recv.at[layer, k - 1]), z * I + flip(j, k), c, False))
            for k in (1, 2, 3)
        ]
        settle(m.d_uppers.at[layer, pl.ds(0, I - 1), 0], m.upper_send.at[layer])

    def up_total(layer):
        if not d.factored:
            land(folds[0, layer])
            value = m.g_up[layer, j].astype(f32)
            for k in range(1, I):
                value += m.up_in[layer, k - 1].astype(f32)
            m.up_sum[layer] = value.astype(bf16)
            return
        for k, made in folds[0, layer]:
            land([made])
            held = m.d_uppers.at[layer, flip(j, k), c]
            for b in range(1, S):
                send(held, held, pair(m.share_sems, layer), pos, section(b), False)
        passed = m.d_uppers.at[layer, pl.ds(0, I - 1), pl.ds(0, S - 1)]
        settle(passed, m.share_sems.at[0, layer])
        arrive(m.others.at[layer, pl.ds(0, I - 1)], m.other_sems.at[1, layer])
        arrive(passed, m.share_sems.at[1, layer])
        value = contract_first(
            m.others[layer].reshape(I * G, d.up_held), m.d_uppers[layer].reshape(I * G, FF)
        )
        m.up_sum[layer] = value.astype(bf16)

    home = q * I + j

    def end_down(layer):
        down_total(layer)
        for a in range(O):
            there = lax.rem(z + a, O)
            source, dest = m.down_sum.at[layer, there], m.down_end.at[zh, q]
            sems = (m.end_down.at[0 if a else 1, layer], m.end_down_recv.at[0])
            if a:
                send(source, dest, sems, column(a), layer, False)
            else:
                deliver(c == layer, source, dest, sems, pos, layer)
        settle(m.down_end.at[0, pl.ds(0, O - 1)], m.end_down.at[0, layer])

    def end_small(layer):
        arrive(m.small_in.at[layer], m.small_fold.at[1, layer])
        value = m.small[layer]
        for k in range(1, I):
            value += m.small_in[layer, k - 1]
        m.small_sum[layer] = value
        for a in range(O):
            source, dest = m.small_sum.at[layer], m.small_end.at[zh, q]
            sems = (m.end_small.at[0 if a else 1, layer], m.end_small_recv.at[0])
            if a:
                send(source, dest, sems, column(a), layer, False)
            else:
                deliver(c == layer, source, dest, sems, pos, layer)
        settle(m.small_end.at[0, pl.ds(0, O - 1)], m.end_small.at[0, layer])

    def end_up(layer):
        up_total(layer)
        sems = (m.end_up.at[layer], m.end_up_recv.at[0])
        mine = jnp.logical_and(c == zh, c == layer)
        deliver(mine, m.up_sum.at[layer], m.up_end.at[zh], sems, home, layer)

    for layer in reversed(range(S)):
        e = S + 1 + layer
        slot = S + layer
        grad = m.grad[...]
        part = contract_last(grad, downs_of(layer))
        middle = trade(e, part, m.cuts.at[slot], m.got.at[slot], m.swap.at[slot])
        if layer + 1 < S:
            refold_down(layer + 1)
        end = middle()
        actives = m.actives[layer].reshape(G, FF)
        m.g_down[layer] = contract_first(actives, grad).astype(bf16).reshape(O, I, d.ff_held, W)
        fold_down(layer)
        if not layer:
            settled = pending[:]
            pending.clear()
        total = end()
        value, factor = m.uppers[layer], m.recips[layer]
        sigm = jax.nn.sigmoid(value)
        d_upper = (total * sigm * (1.0 + value * (1.0 - sigm)) * factor).astype(bf16)
        held = m.d_uppers.at[layer, j if d.factored else 0]
        held[c] = d_upper
        moving = gather(e, held)
        if layer and d.factored:
            share(layer)
        if layer:
            pull = jnp.sum(d_upper.astype(f32) * value, -1, keepdims=True) * factor / d.width
            m.pulls[layer, c] = spread(GS, pull, 0)
            moving += [
                send(
                    m.pulls.at[layer, c],
                    m.pulls.at[layer, c],
                    pair(m.pull_sems, layer, k - 1),
                    pos,
                    section(k),
                )
                for k in range(1, S)
            ]
        land(moving)
        d_all = held[...].reshape(G, FF)
        wide = states[layer].astype(f32)
        d_normed = contract_last(d_all, ups_of(layer))
        m.small[layer, :, :W] = jnp.sum(d_normed * wide, 0, keepdims=True)
        m.small[layer, :, W:] = loss_here
        if layer:
            columns = jnp.concatenate([spread(GS, m.pulls[layer, k], 1) for k in range(S)], 0)
            m.grad[...] = (
                grad.astype(f32) + d_normed * m.gains[layer] - wide * columns
            ).astype(bf16)
        for k in range(1, I):
            sems = pair(m.small_fold, layer)
            send(m.small.at[layer], m.small_in.at[layer, k - 1], sems, z * I + square(k), c, False)
        settle(m.small_in.at[layer], m.small_fold.at[0, layer])
        if not d.factored:
            m.g_up[layer] = contract_first(ready[layer], d_all).astype(bf16).reshape(I, d.up_held, FF)
            fold(0, layer, lambda at: m.g_up.at[layer, at], m.up_in)
        if layer + 1 < S:
            end_up(layer + 1)
            end_small(layer + 1)
            end_down(layer + 1)
    refold_down(0)
    if d.factored:
        share(0)
    drain_columns()
    for finish in settled:
        finish()
    end_down(0)
    end_small(0)
    end_up(0)
    arrive(m.small_end, m.end_small_recv.at[0])
    arrive(m.down_end, m.end_down_recv.at[0])
    lost = jnp.zeros((1, 128), f32)
    for cut in range(O):
        value = jnp.zeros((d.ff_held, W), f32)
        row = jnp.zeros((1, W), f32)
        for h in range(S):
            value += m.down_end[h, cut].astype(f32)
            row += m.small_end[h, cut, :, :W]
            lost += m.small_end[h, cut, :, W:]
        grad_down[:, cut * W : (cut + 1) * W] = value
        grad_gain[:, cut * W : (cut + 1) * W] = row
    loss[...] = lost
    for finish in pending:
        finish()
    value = jnp.zeros((d.up_held, FF), f32)
    arrive(m.up_end, m.end_up_recv.at[0])
    for h in range(S):
        value += m.up_end[h].astype(f32)
    grad_up[...] = value


def on_device(replay, state_ids, sampled, targets, action_table, norm_gain, w_up, w_down):
    held, width = replay.shape
    d = Dims(
        lax.axis_size(SECTION),
        lax.axis_size(DP),
        held,
        width,
        w_up.shape[2],
        action_table.shape[0],
        sampled.shape[1],
        w_up.shape[1],
        w_down.shape[1],
    )
    scratch = scratch_of(d)
    vmem = pl.BlockSpec(memory_space=pltpu.VMEM)
    hbm = pl.BlockSpec(memory_space=pltpu.HBM)
    outs = ((d.up_held, d.ff), (d.ff_held, width), (1, width), (1, 128))
    grad_up, grad_down, grad_gain, loss = pl.pallas_call(
        functools.partial(step_kernel, d, tuple(scratch)),
        out_shape=[jax.ShapeDtypeStruct(shape, f32) for shape in outs],
        in_specs=[hbm, hbm, vmem, vmem, vmem, vmem, vmem, vmem],
        out_specs=[vmem] * 4,
        scratch_shapes=list(scratch.values()),
        compiler_params=pltpu.CompilerParams(
            collective_id=0, has_side_effects=True, vmem_limit_bytes=48 * 1024 * 1024
        ),
    )(
        *(
            pltpu.with_memory_space_constraint(x, pltpu.HBM)
            for x in (
                replay,
                action_table,
                state_ids[None, :],
                sampled.T,
                targets[None, :],
                norm_gain,
                w_up[0],
                w_down[0],
            )
        )
    )
    return (grad_up[None], grad_down[None], grad_gain, loss[0, 0])


def solution(mesh):
    return jax.shard_map(
        on_device,
        mesh=mesh,
        in_specs=(
            P("dp", None),
            P("dp"),
            P("dp", None),
            P("dp"),
            P(),
            P("section", None),
            P("section", "dp", None),
            P("section", "dp", None),
        ),
        out_specs=(P("section", "dp", None), P("section", "dp", None), P("section", None), P()),
        check_vma=False,
    )
```

```python
import functools
import math
import types

import jax
import jax.numpy as jnp
from jax import lax
from jax.experimental import pallas as pl
from jax.experimental.pallas import tpu as pltpu
from jax.sharding import PartitionSpec as P

ROWS_DEV = 128
epsilon = 1e-06
logit_cap = 15.0
bf16 = jnp.bfloat16
f32 = jnp.float32
i32 = jnp.int32
DP, SECTION = "dp", "section"


def contract_last(left, right):
    return lax.dot_general(left, right, (((1,), (1,)), ((), ())), preferred_element_type=f32)


def contract_first(left, right):
    return lax.dot_general(left, right, (((0,), (0,)), ((), ())), preferred_element_type=f32)


def dot(left, right):
    return jnp.dot(left, right, preferred_element_type=f32)


def spread(rows, column, axis):
    here = lax.broadcasted_iota(i32, (rows, rows), 0)
    there = lax.broadcasted_iota(i32, (rows, rows), 1)
    wide = jnp.broadcast_to(column, (rows, rows))
    return jnp.sum(jnp.where(here == there, wide, 0.0), axis, keepdims=True)


def local(source, dest, sem):
    made = pltpu.make_async_copy(source, dest, sem)
    made.start()
    return made


def arrive(dest, sem):
    pltpu.make_async_copy(dest, dest, sem).wait()


def flip(j, k):
    low, high = lax.rem(j, 2), lax.div(j, 2)
    return (2 * (1 - high) if k & 2 else 2 * high) + ((1 - low) if k & 1 else low)


def push(source, dest, sems, dp, section):
    made = pltpu.make_async_remote_copy(
        src_ref=source,
        dst_ref=dest,
        send_sem=sems[0],
        recv_sem=sems[1],
        device_id={DP: dp, SECTION: section},
        device_id_type=pl.DeviceIdType.MESH,
    )
    made.start()
    return made


class Dims:
    def __init__(self, sections, devices, held, width, ff, vocab, samples, up_held, ff_held):
        self.sections, self.devices, self.held, self.width = sections, devices, held, width
        self.ff, self.vocab, self.samples = ff, vocab, samples
        self.up_held, self.ff_held = up_held, ff_held
        self.outer = 2 * sections
        self.inner = devices // self.outer
        self.cut = width // self.outer
        self.group = 2 * held
        self.part = self.group // sections
        self.factored = self.inner == 4 and self.up_held % 128 == 0


def scratch_of(d):
    S, O, I, E = d.sections, d.outer, d.inner, 2 * d.sections + 1
    V, D = pltpu.VMEM, pltpu.SemaphoreType.DMA
    part, cut, ff, held, others = d.part, d.cut, d.ff, d.held, max(S - 1, 1)
    if d.factored:
        kinds = dict(
            others=V((S, I, d.group, d.up_held), bf16),
            down_in=V((S, 6, O // 2, d.ff_held, cut), bf16),
            down_part=V((S, 2, O // 2, d.ff_held, cut), bf16),
            d_uppers=V((S, I, S, part, ff), bf16),
            other_sems=D((2, S)),
            upper_send=D((S,)),
            upper_recv=D((S, I - 1)),
            share_sems=D((2, S)),
            half_send=D((S,)),
            half_recv=D((S, 3)),
        )
    else:
        kinds = dict(
            g_up=V((S, I, d.up_held, ff), bf16),
            up_in=V((S, I - 1, d.up_held, ff), bf16),
            down_in=V((S, I - 1, O, d.ff_held, cut), bf16),
            d_uppers=V((S, 1, S, part, ff), bf16),
            fold=D((2, 2, S, I - 1)),
        )
    return dict(
        **kinds,
        rep=V((2, held, cut), bf16),
        tab=V((2, d.vocab, cut), bf16),
        gains=V((S, 1, cut), f32),
        ups=V((S, I, d.up_held, ff), bf16),
        downs=V((S, O, I, d.ff_held, cut), bf16),
        away=V((held, cut), bf16),
        states=V((S + 1, d.group, cut), bf16),
        ready=V((S, d.group, cut), bf16),
        picks=V((2, d.samples, held), i32),
        marks=V((2, 1, held), i32),
        counts=V((held, d.vocab), f32),
        hots=V((held, d.vocab), f32),
        acc=V((S, part, ff), f32),
        cuts=V((2 * S, S, part, ff), bf16),
        got=V((2 * S, S, part, ff), bf16),
        swap=V((2 * S, 2, part, ff), bf16),
        score_cuts=V((S, part, d.vocab), f32),
        score_got=V((S, part, d.vocab), f32),
        score_swap=V((2, part, d.vocab), bf16),
        stat_cuts=V((S, S, 1, part), f32),
        stat_got=V((S, S, 1, part), f32),
        stat_swap=V((S, 2, 1, part), f32),
        uppers=V((S, part, ff), f32),
        recips=V((S, part, 1), f32),
        actives=V((S, S, part, ff), bf16),
        d_all=V((S, part, d.vocab), bf16),
        pulls=V((S, S, 1, part), f32),
        grad=V((d.group, cut), bf16),
        g_down=V((S, O, I, d.ff_held, cut), bf16),
        up_sum=V((S, d.up_held, ff), bf16),
        down_sum=V((S, O, d.ff_held, cut), bf16),
        small=V((S, 1, cut + 128), f32),
        small_in=V((S, I - 1, 1, cut + 128), f32),
        small_sum=V((S, 1, cut + 128), f32),
        load_sems=D((4,)),
        gain_sems=D((2, S)),
        start_sems=D((3, 2)),
        col_up=D((2, S)),
        col_down=D((S,)),
        send_down=D((2,)),
        square_send=D((2, S)),
        square_recv=D((2, S, I - 1)),
        trade=D((2, E, 3, others)),
        tallies=D((2, S, 2, others)),
        pull_sems=D((2, S, others)),
        small_fold=D((2, S)),
        end_up=D((S,)),
        end_up_recv=D((1,)),
        end_down=D((2, S)),
        end_down_recv=D((1,)),
        end_small=D((2, S)),
        end_small_recv=D((1,)),
    )


def step_kernel(d, names, *refs):
    ins, outs, held_refs = refs[:8], refs[8:11], refs[11:]
    replay, table, ids, sampled, targets, gain, up, down = ins
    m = types.SimpleNamespace(**dict(zip(names, held_refs)))
    m.up_end, m.down_end, m.small_end = outs
    S, O, I, W, R, FF, V = d.sections, d.outer, d.inner, d.cut, d.held, d.ff, d.vocab
    GS, G = d.part, d.group
    scale = math.sqrt(d.width)
    c = lax.axis_index(SECTION)
    pos = lax.axis_index(DP)
    z, j = lax.div(pos, I), lax.rem(pos, I)
    zh, p = lax.div(z, 2), lax.rem(z, 2)
    q = 2 * c + p
    partner = (z + 1 - 2 * p) * I + j
    ups, downs, states, ready = m.ups, m.downs, m.states, m.ready
    pending = []

    def column(k):
        return lax.rem(z + k, O) * I + j

    def section(k):
        return lax.rem(c + k, S)

    def square(k):
        return lax.rem(j + k, I)

    def pair(held, *at):
        return held.at[(0, *at)], held.at[(1, *at)]

    def send(source, dest, sems, dp, to, track=True):
        made = push(source, dest, sems, dp, to)
        if track:
            pending.append(made.wait_send)
        return made

    def settle(span, sem):
        pending.append(lambda: arrive(span, sem))

    def deliver(mine, source, dest, sems, dp, to, track=True):
        @pl.when(mine)
        def _():
            local(source, dest, sems[1])

        @pl.when(jnp.logical_not(mine))
        def _():
            push(source, dest, sems, dp, to)

        def finish():
            @pl.when(jnp.logical_not(mine))
            def _():
                arrive(source, sems[0])

        if track:
            pending.append(finish)

    def cut_of(n):
        return pl.ds(pl.multiple_of(n * W, W), W)

    other = 2 * c + 1 - p
    loads = []
    for n, at in ((0, other), (1, q)):
        loads.append(local(replay.at[:, cut_of(at)], m.rep.at[n], m.load_sems.at[n]))
        loads.append(local(table.at[:, cut_of(at)], m.tab.at[n], m.load_sems.at[2 + n]))

    barrier = pltpu.get_barrier_semaphore()
    peers = [(column(a), section(b)) for a in range(O) for b in range(S) if a or b]
    peers += [(z * I + square(k), c) for k in range(1, I)]
    for dp, to in peers:
        pl.semaphore_signal(
            barrier, inc=1, device_id={DP: dp, SECTION: to}, device_id_type=pl.DeviceIdType.MESH
        )
    pl.semaphore_wait(barrier, len(peers))

    def up_column():
        for k in range(S):
            home = (2 * lax.rem(zh + k, S) + p) * I + j
            sems = (m.col_up.at[0, k], m.col_up.at[1, c])
            if k == 0:
                deliver(c == zh, up, ups.at[c, j], sems, home, zh, False)
            else:
                push(up, ups.at[c, j], sems, home, zh)

    def down_column():
        for a in range(O):
            for b in range(S):
                there = lax.rem(z + a, O)
                piece = down.at[:, cut_of(2 * section(b) + lax.rem(there, 2))]
                dest = downs.at[c, z, j]
                if a or b:
                    sems = (m.send_down.at[0 if a else 1], m.col_down.at[c])
                    push(piece, dest, sems, column(a), section(b))
                else:
                    local(piece, dest, m.col_down.at[c])

    def drain_columns():
        @pl.when(c != zh)
        def _():
            arrive(up, m.col_up.at[0, 0])

        for k in range(1, S):
            arrive(up, m.col_up.at[0, k])
        arrive(downs.at[:, pl.ds(0, O - 1), 0], m.send_down.at[0])
        if S > 1:
            arrive(downs.at[pl.ds(0, S - 1), 0, 0], m.send_down.at[1])

    first = c == 0
    later = c != 0
    extra = [
        send(sampled, m.picks.at[p], (m.start_sems.at[0, 0], m.start_sems.at[0, 1]), partner, c),
        send(targets, m.marks.at[p], (m.start_sems.at[1, 0], m.start_sems.at[1, 1]), partner, c),
    ]

    @pl.when(first)
    def _():
        up_column()
        down_column()

    for k in range(1, S):
        sems = pair(m.gain_sems, k)
        send(gain.at[:, cut_of(2 * section(k) + p)], m.gains.at[c], sems, pos, section(k))
    local(gain.at[:, cut_of(q)], m.gains.at[c], m.gain_sems.at[1, 0])

    id_hot = (lax.broadcasted_iota(i32, (R, R), 0) == ids[...] - pos * R).astype(bf16)
    taken = (lax.broadcasted_iota(i32, (V, R), 0) == sampled[0:1]).astype(bf16)
    for n in range(2):
        loads[2 * n].wait()
        loads[2 * n + 1].wait()
        start = (contract_first(id_hot, m.rep[n]) + contract_first(taken, m.tab[n])).astype(bf16)
        mine_rows = pl.ds(pl.multiple_of(p * R, R), R)
        if n == 0:
            m.away[...] = start
            sems = (m.start_sems.at[2, 0], m.start_sems.at[2, 1])
            moved = send(m.away, states.at[0, mine_rows], sems, partner, c)
        else:
            states[0, mine_rows] = start

    chip, row = lax.div(c * GS, R), pl.multiple_of(lax.rem(c * GS, R), GS)

    def count():
        m.marks[p] = targets[...]
        m.picks[p] = sampled[...]
        land(extra)
        picks, marks = m.picks[chip], m.marks[chip]
        actions = lax.broadcasted_iota(i32, (V, R), 0)
        counts, hots = jnp.zeros((V, R), f32), jnp.zeros((V, R), f32)
        for k in range(d.samples):
            hit = jnp.where(picks[k : k + 1] == actions, 1.0, 0.0)
            counts += hit
            hots += jnp.where(marks == k, hit, 0.0)
        m.counts[...] = counts.T
        m.hots[...] = hots.T

    fans = {}
    relayed = I == 4

    def block(kind, layer, at, half=None):
        if kind == 0:
            if half is None:
                return ups.at[layer, at]
            return ups.at[layer, at, pl.ds(half * (d.up_held // 2), d.up_held // 2)]
        if half is None:
            return downs.at[layer, :, at]
        return downs.at[layer, pl.ds(half * (O // 2), O // 2), at]

    def blocks(kind, layer, n):
        return ups.at[layer, pl.ds(0, n)] if kind == 0 else downs.at[layer, :, pl.ds(0, n)]

    def fan(kind, layer):
        if kind == 0:
            arrive(ups.at[layer, j], m.col_up.at[1, layer])
        else:
            arrive(downs.at[layer, :, j], m.col_down.at[layer])
        going, coming = m.square_send.at[kind, layer], m.square_recv.at[kind, layer]
        made = fans[kind, layer] = {}
        if relayed:
            for k, half, n in ((1, 0, 0), (2, 1, 1), (1, 1, 2), (2, 0, 2)):
                view = block(kind, layer, j, half)
                to = z * I + flip(j, k)
                made[n] = send(view, view, (going, coming.at[n]), to, c, False)
        else:
            view = block(kind, layer, j)
            for k in range(1, I):
                to = z * I + square(k)
                made[k] = send(view, view, (going, coming.at[k - 1]), to, c, False)
        settle(blocks(kind, layer, I - 1), going)

    def relay(kind, layer):
        if relayed:
            made = fans[kind, layer]
            going, coming = m.square_send.at[kind, layer], m.square_recv.at[kind, layer]
            for k, half in ((1, 0), (2, 1)):
                land([made[half]])
                view = block(kind, layer, flip(j, k), half)
                send(view, view, (going, coming.at[2]), z * I + flip(j, 3 - k), c, False)

    def land_fan(kind, layer):
        if relayed:
            arrive(blocks(kind, layer, 2), m.square_recv.at[kind, layer, 2])
        else:
            land(fans[kind, layer])

    def land(made):
        for copy in made.values() if isinstance(made, dict) else made:
            copy.wait_recv()

    def tally(e, slot, stat):
        for k in range(S):
            m.stat_cuts[slot, k] = spread(GS, stat[k * GS : (k + 1) * GS], 0)
        rows = [
            send(
                m.stat_cuts.at[slot, section(k)],
                m.stat_got.at[slot, k],
                pair(m.tallies, slot, 0, k - 1),
                pos,
                section(k),
            )
            for k in range(1, S)
        ]

        def finish():
            land(rows)
            row = m.stat_cuts[slot, c]
            for k in range(1, S):
                row += m.stat_got[slot, k]
            m.stat_swap[slot, 0] = row
            swap = m.stat_swap.at[slot]
            over = send(swap.at[0], swap.at[1], pair(m.tallies, slot, 1, 0), partner, c)

            def end():
                land([over])
                return spread(GS, row + m.stat_swap[slot, 1], 1)

            return end

        return finish

    def trade(e, partial, cuts, got, swap):
        m_acc = m.acc
        span = partial.shape[1]
        split = partial.reshape(S, GS, span)
        m_acc[:, :, :span] = split
        cuts[...] = split.astype(cuts.dtype)
        sent = [
            send(cuts.at[section(k)], got.at[k], pair(m.trade, e, 0, k - 1), pos, section(k))
            for k in range(1, S)
        ]

        def finish():
            land(sent)
            total = m_acc[c, :, :span]
            for k in range(1, S):
                total += got[k].astype(f32)
            swap[0] = total.astype(swap.dtype)
            over = send(swap.at[0], swap.at[1], pair(m.trade, e, 1, 0), partner, c)

            def end():
                land([over])
                return total + swap[1].astype(f32)

            return end

        return finish

    def gather(e, held):
        return [
            send(held.at[c], held.at[c], pair(m.trade, e, 2, k - 1), pos, section(k))
            for k in range(1, S)
        ]

    fan(0, 0)
    count()
    relay(0, 0)
    fan(1, 0)
    pl.when(later)(up_column)
    moved.wait_recv()
    arrive(m.gains.at[c], m.gain_sems.at[1, 0])
    for k in range(1, S):
        giver = lax.rem(c + S - k, S)
        arrive(m.gains.at[giver], m.gain_sems.at[1, k])

    def lend(layer):
        if d.factored:
            own = pl.ds(pl.multiple_of(j * d.up_held, 128), d.up_held)
            m.others[layer, j] = ready[layer, :, own]
            for k in (1, 2, 3):
                send(
                    ready.at[layer, :, pl.ds(pl.multiple_of(flip(j, k) * d.up_held, 128), d.up_held)],
                    m.others.at[layer, j],
                    pair(m.other_sems, layer),
                    z * I + flip(j, k),
                    c,
                    False,
                )
            settle(m.others.at[layer, pl.ds(0, I - 1)], m.other_sems.at[0, layer])

    def ups_of(layer):
        return ups[layer].reshape(W, FF)

    def downs_of(layer):
        return downs[layer].reshape(FF, W)

    for layer in range(S):
        wide = states[layer].astype(f32)
        ready[layer] = (wide * m.gains[layer]).astype(bf16)
        counted = tally(layer, layer, jnp.sum(wide * wide, -1, keepdims=True))
        land_fan(0, layer)
        partial = dot(ready[layer], ups_of(layer))
        middle = trade(layer, partial, m.cuts.at[layer], m.got.at[layer], m.swap.at[layer])
        counted = counted()
        if layer == 0:
            pl.when(later)(down_column)
        relay(1, layer)
        if layer + 1 == S:
            for held_layer in range(S):
                lend(held_layer)
        end = middle()
        if layer + 1 < S:
            fan(0, layer + 1)
        factor = lax.rsqrt(counted() / d.width + epsilon)
        value = end() * factor
        m.uppers[layer] = value
        m.recips[layer] = factor
        held = m.actives.at[layer]
        held[c] = (value * jax.nn.sigmoid(value)).astype(bf16)
        moving = gather(layer, held)
        if layer + 1 < S:
            relay(0, layer + 1)
            fan(1, layer + 1)
        land_fan(1, layer)
        land(moving)
        states[layer + 1] = (
            states[layer].astype(f32) + dot(m.actives[layer].reshape(G, FF), downs_of(layer))
        ).astype(bf16)

    part = contract_last(states[S], m.tab[1])
    total = trade(S, part, m.score_cuts, m.score_got, m.score_swap)()()
    bent = jnp.tanh(total / scale / logit_cap)
    logits = logit_cap * bent
    counts, hots = m.counts[pl.ds(row, GS)], m.hots[pl.ds(row, GS)]
    weighted = counts * jnp.exp(logits)
    summed = jnp.sum(weighted, -1, keepdims=True)
    d_scores = (weighted / summed - hots) / ROWS_DEV * (1.0 - bent * bent) / scale
    m.d_all[c] = d_scores.astype(bf16)
    moving = gather(S, m.d_all)
    cross = jnp.log(summed) - jnp.sum(logits * hots, -1, keepdims=True)
    counted = jnp.where(p == 0, 1.0 / ROWS_DEV, 0.0)
    loss_here = jnp.broadcast_to(jnp.sum(cross, 0, keepdims=True) * counted, (1, 128))
    land(moving)
    m.grad[...] = dot(m.d_all[...].reshape(G, V), m.tab[1]).astype(bf16)

    folds = {}

    def fold(kind, layer, source, dest):
        folds[kind, layer] = [
            send(source(square(k)), dest.at[layer, k - 1], pair(m.fold, kind, layer, k - 1), z * I + square(k), c)
            for k in range(1, I)
        ]

    def fold_down(layer):
        if not d.factored:
            fold(1, layer, lambda at: m.g_down.at[layer, :, at], m.down_in)
            return
        made = folds[1, layer] = {}
        for n, k, at, half in ((1, 1, 3, 0), (3, 2, 3, 1), (0, 1, 1, 0), (2, 2, 2, 1)):
            source = m.g_down.at[layer, pl.ds(half * (O // 2), O // 2), flip(j, at)]
            sems = (m.half_send.at[layer], m.half_recv.at[layer, {1: 0, 3: 1}.get(n, 2)])
            made[n] = send(source, m.down_in.at[layer, n], sems, z * I + flip(j, k), c, False)

    def refold_down(layer):
        if not d.factored:
            return
        made = folds[1, layer]
        for n, k, half in ((1, 2, 0), (3, 1, 1)):
            land([made[n]])
            own = m.g_down[layer, half * (O // 2) : (half + 1) * (O // 2), flip(j, k)]
            into = m.down_part.at[layer, half]
            into[...] = (own.astype(f32) + m.down_in[layer, n].astype(f32)).astype(bf16)
            sems = (m.half_send.at[layer], m.half_recv.at[layer, 2])
            send(into, m.down_in.at[layer, 4 + half], sems, z * I + flip(j, k), c, False)
        settle(m.down_in.at[layer], m.half_send.at[layer])

    def down_total(layer):
        if not d.factored:
            land(folds[1, layer])
            value = m.g_down[layer, :, j].astype(f32)
            for k in range(1, I):
                value += m.down_in[layer, k - 1].astype(f32)
            m.down_sum[layer] = value.astype(bf16)
            return
        arrive(m.down_in.at[layer, pl.ds(0, 4)], m.half_recv.at[layer, 2])
        for half in range(2):
            rows = pl.ds(half * (O // 2), O // 2)
            value = m.g_down[layer, rows, j].astype(f32)
            for n in (2 * half, 4 + half):
                value += m.down_in[layer, n].astype(f32)
            m.down_sum[layer, rows] = value.astype(bf16)

    def share(layer):
        held = m.d_uppers.at[layer, j, c]
        folds[0, layer] = [
            (k, send(held, held, (m.upper_send.at[layer], m.upper_recv.at[layer, k - 1]), z * I + flip(j, k), c, False))
            for k in (1, 2, 3)
        ]
        settle(m.d_uppers.at[layer, pl.ds(0, I - 1), 0], m.upper_send.at[layer])

    def up_total(layer):
        if not d.factored:
            land(folds[0, layer])
            value = m.g_up[layer, j].astype(f32)
            for k in range(1, I):
                value += m.up_in[layer, k - 1].astype(f32)
            m.up_sum[layer] = value.astype(bf16)
            return
        for k, made in folds[0, layer]:
            land([made])
            held = m.d_uppers.at[layer, flip(j, k), c]
            for b in range(1, S):
                send(held, held, pair(m.share_sems, layer), pos, section(b), False)
        passed = m.d_uppers.at[layer, pl.ds(0, I - 1), pl.ds(0, S - 1)]
        settle(passed, m.share_sems.at[0, layer])
        arrive(m.others.at[layer, pl.ds(0, I - 1)], m.other_sems.at[1, layer])
        arrive(passed, m.share_sems.at[1, layer])
        value = contract_first(
            m.others[layer].reshape(I * G, d.up_held), m.d_uppers[layer].reshape(I * G, FF)
        )
        m.up_sum[layer] = value.astype(bf16)

    home = q * I + j

    def end_down(layer):
        down_total(layer)
        for a in range(O):
            there = lax.rem(z + a, O)
            source, dest = m.down_sum.at[layer, there], m.down_end.at[zh, q]
            sems = (m.end_down.at[0 if a else 1, layer], m.end_down_recv.at[0])
            if a:
                send(source, dest, sems, column(a), layer, False)
            else:
                deliver(c == layer, source, dest, sems, pos, layer)
        settle(m.down_end.at[0, pl.ds(0, O - 1)], m.end_down.at[0, layer])

    def end_small(layer):
        arrive(m.small_in.at[layer], m.small_fold.at[1, layer])
        value = m.small[layer]
        for k in range(1, I):
            value += m.small_in[layer, k - 1]
        m.small_sum[layer] = value
        for a in range(O):
            source, dest = m.small_sum.at[layer], m.small_end.at[zh, q]
            sems = (m.end_small.at[0 if a else 1, layer], m.end_small_recv.at[0])
            if a:
                send(source, dest, sems, column(a), layer, False)
            else:
                deliver(c == layer, source, dest, sems, pos, layer)
        settle(m.small_end.at[0, pl.ds(0, O - 1)], m.end_small.at[0, layer])

    def end_up(layer):
        up_total(layer)
        sems = (m.end_up.at[layer], m.end_up_recv.at[0])
        mine = jnp.logical_and(c == zh, c == layer)
        deliver(mine, m.up_sum.at[layer], m.up_end.at[zh], sems, home, layer)

    for layer in reversed(range(S)):
        e = S + 1 + layer
        slot = S + layer
        grad = m.grad[...]
        part = contract_last(grad, downs_of(layer))
        middle = trade(e, part, m.cuts.at[slot], m.got.at[slot], m.swap.at[slot])
        if layer + 1 < S:
            refold_down(layer + 1)
        end = middle()
        actives = m.actives[layer].reshape(G, FF)
        m.g_down[layer] = contract_first(actives, grad).astype(bf16).reshape(O, I, d.ff_held, W)
        fold_down(layer)
        if not layer:
            settled = pending[:]
            pending.clear()
        total = end()
        value, factor = m.uppers[layer], m.recips[layer]
        sigm = jax.nn.sigmoid(value)
        d_upper = (total * sigm * (1.0 + value * (1.0 - sigm)) * factor).astype(bf16)
        held = m.d_uppers.at[layer, j if d.factored else 0]
        held[c] = d_upper
        moving = gather(e, held)
        if layer and d.factored:
            share(layer)
        if layer:
            pull = jnp.sum(d_upper.astype(f32) * value, -1, keepdims=True) * factor / d.width
            m.pulls[layer, c] = spread(GS, pull, 0)
            moving += [
                send(
                    m.pulls.at[layer, c],
                    m.pulls.at[layer, c],
                    pair(m.pull_sems, layer, k - 1),
                    pos,
                    section(k),
                )
                for k in range(1, S)
            ]
        land(moving)
        d_all = held[...].reshape(G, FF)
        wide = states[layer].astype(f32)
        d_normed = contract_last(d_all, ups_of(layer))
        m.small[layer, :, :W] = jnp.sum(d_normed * wide, 0, keepdims=True)
        m.small[layer, :, W:] = loss_here
        if layer:
            columns = jnp.concatenate([spread(GS, m.pulls[layer, k], 1) for k in range(S)], 0)
            m.grad[...] = (
                grad.astype(f32) + d_normed * m.gains[layer] - wide * columns
            ).astype(bf16)
        for k in range(1, I):
            sems = pair(m.small_fold, layer)
            send(m.small.at[layer], m.small_in.at[layer, k - 1], sems, z * I + square(k), c, False)
        settle(m.small_in.at[layer], m.small_fold.at[0, layer])
        if not d.factored:
            m.g_up[layer] = contract_first(ready[layer], d_all).astype(bf16).reshape(I, d.up_held, FF)
            fold(0, layer, lambda at: m.g_up.at[layer, at], m.up_in)
        if layer + 1 < S:
            end_up(layer + 1)
            end_small(layer + 1)
            end_down(layer + 1)
    refold_down(0)
    if d.factored:
        share(0)
    drain_columns()
    for finish in settled:
        finish()
    end_down(0)
    end_small(0)
    end_up(0)
    arrive(m.small_end, m.end_small_recv.at[0])
    arrive(m.down_end, m.end_down_recv.at[0])
    for finish in pending:
        finish()
    arrive(m.up_end, m.end_up_recv.at[0])


def sum_kernel(d, up_end, down_end, small_end, grad_up, grad_down, grad_gain, loss):
    W = d.cut

    def total(pieces):
        value = pieces[0].astype(f32)
        for piece in pieces[1:]:
            value += piece.astype(f32)
        return value

    groups = range(d.sections)
    lost = []
    grad_up[...] = total([up_end[h] for h in groups])
    for cut in range(d.outer):
        at = slice(cut * W, (cut + 1) * W)
        grad_down[:, at] = total([down_end[h, cut] for h in groups])
        grad_gain[:, at] = total([small_end[h, cut, :, :W] for h in groups])
        lost += [small_end[h, cut, :, W:] for h in groups]
    loss[0, 0] = total(lost)[0, 0]


def on_device(replay, state_ids, sampled, targets, action_table, norm_gain, w_up, w_down):
    held, width = replay.shape
    d = Dims(
        lax.axis_size(SECTION),
        lax.axis_size(DP),
        held,
        width,
        w_up.shape[2],
        action_table.shape[0],
        sampled.shape[1],
        w_up.shape[1],
        w_down.shape[1],
    )
    scratch = scratch_of(d)
    vmem = pl.BlockSpec(memory_space=pltpu.VMEM)
    hbm = pl.BlockSpec(memory_space=pltpu.HBM)
    ends = (
        jax.ShapeDtypeStruct((d.sections, d.up_held, d.ff), bf16),
        jax.ShapeDtypeStruct((d.sections, d.outer, d.ff_held, d.cut), bf16),
        jax.ShapeDtypeStruct((d.sections, d.outer, 1, d.cut + 128), f32),
    )
    parts = pl.pallas_call(
        functools.partial(step_kernel, d, tuple(scratch)),
        out_shape=ends,
        in_specs=[hbm, hbm, vmem, vmem, vmem, vmem, vmem, vmem],
        out_specs=[vmem] * 3,
        scratch_shapes=list(scratch.values()),
        compiler_params=pltpu.CompilerParams(
            collective_id=0, has_side_effects=True, vmem_limit_bytes=48 * 1024 * 1024
        ),
    )(
        *(
            pltpu.with_memory_space_constraint(x, pltpu.HBM)
            for x in (
                replay,
                action_table,
                state_ids[None, :],
                sampled.T,
                targets[None, :],
                norm_gain,
                w_up[0],
                w_down[0],
            )
        )
    )
    outs = ((d.up_held, d.ff), (d.ff_held, width), (1, width), (1, 1))
    grad_up, grad_down, grad_gain, loss = pl.pallas_call(
        functools.partial(sum_kernel, d),
        out_shape=[jax.ShapeDtypeStruct(shape, f32) for shape in outs],
        in_specs=[vmem] * 3,
        out_specs=[vmem] * 3 + [pl.BlockSpec(memory_space=pltpu.SMEM)],
        compiler_params=pltpu.CompilerParams(vmem_limit_bytes=8 * 1024 * 1024),
    )(*parts)
    return (grad_up[None], grad_down[None], grad_gain, loss.reshape(()))


def solution(mesh):
    return jax.shard_map(
        on_device,
        mesh=mesh,
        in_specs=(
            P("dp", None),
            P("dp"),
            P("dp", None),
            P("dp"),
            P(),
            P("section", None),
            P("section", "dp", None),
            P("section", "dp", None),
        ),
        out_specs=(P("section", "dp", None), P("section", "dp", None), P("section", None), P()),
        check_vma=False,
    )
```

```python
import functools
import math
import types

import jax
import jax.numpy as jnp
from jax import lax
from jax.experimental import pallas as pl
from jax.experimental.pallas import tpu as pltpu
from jax.sharding import PartitionSpec as P

ROWS_DEV = 128
epsilon = 1e-06
logit_cap = 15.0
bf16 = jnp.bfloat16
f32 = jnp.float32
i32 = jnp.int32
DP, SECTION = "dp", "section"


def contract_last(left, right):
    return lax.dot_general(left, right, (((1,), (1,)), ((), ())), preferred_element_type=f32)


def contract_first(left, right):
    return lax.dot_general(left, right, (((0,), (0,)), ((), ())), preferred_element_type=f32)


def dot(left, right):
    return jnp.dot(left, right, preferred_element_type=f32)


def spread(rows, column, axis):
    here = lax.broadcasted_iota(i32, (rows, rows), 0)
    there = lax.broadcasted_iota(i32, (rows, rows), 1)
    wide = jnp.broadcast_to(column, (rows, rows))
    return jnp.sum(jnp.where(here == there, wide, 0.0), axis, keepdims=True)


def local(source, dest, sem):
    made = pltpu.make_async_copy(source, dest, sem)
    made.start()
    return made


def arrive(dest, sem):
    pltpu.make_async_copy(dest, dest, sem).wait()


def flip(j, k):
    low, high = lax.rem(j, 2), lax.div(j, 2)
    return (2 * (1 - high) if k & 2 else 2 * high) + ((1 - low) if k & 1 else low)


def push(source, dest, sems, dp, section):
    made = pltpu.make_async_remote_copy(
        src_ref=source,
        dst_ref=dest,
        send_sem=sems[0],
        recv_sem=sems[1],
        device_id={DP: dp, SECTION: section},
        device_id_type=pl.DeviceIdType.MESH,
    )
    made.start()
    return made


class Dims:
    def __init__(self, sections, devices, held, width, ff, vocab, samples, up_held, ff_held):
        self.sections, self.devices, self.held, self.width = sections, devices, held, width
        self.ff, self.vocab, self.samples = ff, vocab, samples
        self.up_held, self.ff_held = up_held, ff_held
        self.outer = 2 * sections
        self.inner = devices // self.outer
        self.cut = width // self.outer
        self.group = 2 * held
        self.part = self.group // sections
        self.factored = self.inner == 4 and self.up_held % 128 == 0


def scratch_of(d):
    S, O, I, E = d.sections, d.outer, d.inner, 2 * d.sections + 1
    V, D = pltpu.VMEM, pltpu.SemaphoreType.DMA
    part, cut, ff, held, others = d.part, d.cut, d.ff, d.held, max(S - 1, 1)
    if d.factored:
        kinds = dict(
            others=V((S, I, d.group, d.up_held), bf16),
            down_in=V((S, 6, O // 2, d.ff_held, cut), bf16),
            down_part=V((S, 2, O // 2, d.ff_held, cut), bf16),
            d_uppers=V((S, I, S, part, ff), bf16),
            other_sems=D((2, S)),
            upper_send=D((S,)),
            upper_recv=D((S, I - 1)),
            share_sems=D((2, S)),
            half_send=D((S,)),
            half_recv=D((S, 3)),
        )
    else:
        kinds = dict(
            g_up=V((S, I, d.up_held, ff), bf16),
            up_in=V((S, I - 1, d.up_held, ff), bf16),
            down_in=V((S, I - 1, O, d.ff_held, cut), bf16),
            d_uppers=V((S, 1, S, part, ff), bf16),
            fold=D((2, 2, S, I - 1)),
        )
    return dict(
        **kinds,
        ids=V((1, held), i32),
        sampled=V((d.samples, held), i32),
        targets=V((1, held), i32),
        gain=V((1, d.width), f32),
        up=V((d.up_held, ff), bf16),
        down=V((d.ff_held, d.width), bf16),
        rep=V((2, held, cut), bf16),
        tab=V((2, d.vocab, cut), bf16),
        gains=V((S, 1, cut), f32),
        ups=V((S, I, d.up_held, ff), bf16),
        downs=V((S, O, I, d.ff_held, cut), bf16),
        away=V((held, cut), bf16),
        states=V((S + 1, d.group, cut), bf16),
        ready=V((S, d.group, cut), bf16),
        picks=V((2, d.samples, held), i32),
        marks=V((2, 1, held), i32),
        counts=V((held, d.vocab), f32),
        hots=V((held, d.vocab), f32),
        acc=V((S, part, ff), f32),
        cuts=V((2 * S, S, part, ff), bf16),
        got=V((2 * S, S, part, ff), bf16),
        swap=V((2 * S, 2, part, ff), bf16),
        score_cuts=V((S, part, d.vocab), f32),
        score_got=V((S, part, d.vocab), f32),
        score_swap=V((2, part, d.vocab), bf16),
        stat_cuts=V((S, S, 1, part), f32),
        stat_got=V((S, S, 1, part), f32),
        stat_swap=V((S, 2, 1, part), f32),
        uppers=V((S, part, ff), f32),
        recips=V((S, part, 1), f32),
        actives=V((S, S, part, ff), bf16),
        d_all=V((S, part, d.vocab), bf16),
        pulls=V((S, S, 1, part), f32),
        grad=V((d.group, cut), bf16),
        g_down=V((S, O, I, d.ff_held, cut), bf16),
        up_sum=V((S, d.up_held, ff), bf16),
        down_sum=V((S, O, d.ff_held, cut), bf16),
        small=V((S, 1, cut + 128), f32),
        small_in=V((S, I - 1, 1, cut + 128), f32),
        small_sum=V((S, 1, cut + 128), f32),
        load_sems=D((4,)),
        first_sems=D((6,)),
        gain_sems=D((2, S)),
        start_sems=D((3, 2)),
        col_up=D((2, S)),
        col_down=D((S,)),
        send_down=D((2,)),
        square_send=D((2, S)),
        square_recv=D((2, S, I - 1)),
        trade=D((2, E, 3, others)),
        tallies=D((2, S, 2, others)),
        pull_sems=D((2, S, others)),
        small_fold=D((2, S)),
        end_up=D((S,)),
        end_up_recv=D((1,)),
        end_down=D((2, S)),
        end_down_recv=D((1,)),
        end_small=D((2, S)),
        end_small_recv=D((1,)),
    )


def step_kernel(d, names, *refs):
    ins, outs, held_refs = refs[:8], refs[8:11], refs[11:]
    replay, table, *firsts = ins
    m = types.SimpleNamespace(**dict(zip(names, held_refs)))
    m.up_end, m.down_end, m.small_end = outs
    ids, sampled, targets, gain, up, down = kept = m.ids, m.sampled, m.targets, m.gain, m.up, m.down
    S, O, I, W, R, FF, V = d.sections, d.outer, d.inner, d.cut, d.held, d.ff, d.vocab
    GS, G = d.part, d.group
    scale = math.sqrt(d.width)
    c = lax.axis_index(SECTION)
    pos = lax.axis_index(DP)
    z, j = lax.div(pos, I), lax.rem(pos, I)
    zh, p = lax.div(z, 2), lax.rem(z, 2)
    q = 2 * c + p
    partner = (z + 1 - 2 * p) * I + j
    ups, downs, states, ready = m.ups, m.downs, m.states, m.ready
    pending = []

    def column(k):
        return lax.rem(z + k, O) * I + j

    def section(k):
        return lax.rem(c + k, S)

    def square(k):
        return lax.rem(j + k, I)

    def pair(held, *at):
        return held.at[(0, *at)], held.at[(1, *at)]

    def send(source, dest, sems, dp, to, track=True):
        made = push(source, dest, sems, dp, to)
        if track:
            pending.append(made.wait_send)
        return made

    def settle(span, sem):
        pending.append(lambda: arrive(span, sem))

    def deliver(mine, source, dest, sems, dp, to, track=True):
        @pl.when(mine)
        def _():
            local(source, dest, sems[1])

        @pl.when(jnp.logical_not(mine))
        def _():
            push(source, dest, sems, dp, to)

        def finish():
            @pl.when(jnp.logical_not(mine))
            def _():
                arrive(source, sems[0])

        if track:
            pending.append(finish)

    def cut_of(n):
        return pl.ds(pl.multiple_of(n * W, W), W)

    barrier = pltpu.get_barrier_semaphore()
    peers = [(column(a), section(b)) for a in range(O) for b in range(S) if a or b]
    peers += [(z * I + square(k), c) for k in range(1, I)]
    for dp, to in peers:
        pl.semaphore_signal(
            barrier, inc=1, device_id={DP: dp, SECTION: to}, device_id_type=pl.DeviceIdType.MESH
        )
    early = [local(firsts[n], kept[n], m.first_sems.at[n]) for n in (3, 2, 4, 5, 1, 0)]
    other = 2 * c + 1 - p
    loads = []
    for n, at in ((0, other), (1, q)):
        loads.append(local(replay.at[:, cut_of(at)], m.rep.at[n], m.load_sems.at[n]))
        loads.append(local(table.at[:, cut_of(at)], m.tab.at[n], m.load_sems.at[2 + n]))
    pl.semaphore_wait(barrier, len(peers))
    for copy in early:
        copy.wait()

    def up_column():
        for k in range(S):
            home = (2 * lax.rem(zh + k, S) + p) * I + j
            sems = (m.col_up.at[0, k], m.col_up.at[1, c])
            if k == 0:
                deliver(c == zh, up, ups.at[c, j], sems, home, zh, False)
            else:
                push(up, ups.at[c, j], sems, home, zh)

    def down_column():
        for a in range(O):
            for b in range(S):
                there = lax.rem(z + a, O)
                piece = down.at[:, cut_of(2 * section(b) + lax.rem(there, 2))]
                dest = downs.at[c, z, j]
                if a or b:
                    sems = (m.send_down.at[0 if a else 1], m.col_down.at[c])
                    push(piece, dest, sems, column(a), section(b))
                else:
                    local(piece, dest, m.col_down.at[c])

    def drain_columns():
        @pl.when(c != zh)
        def _():
            arrive(up, m.col_up.at[0, 0])

        for k in range(1, S):
            arrive(up, m.col_up.at[0, k])
        arrive(downs.at[:, pl.ds(0, O - 1), 0], m.send_down.at[0])
        if S > 1:
            arrive(downs.at[pl.ds(0, S - 1), 0, 0], m.send_down.at[1])

    first = c == 0
    later = c != 0
    extra = [
        send(sampled, m.picks.at[p], (m.start_sems.at[0, 0], m.start_sems.at[0, 1]), partner, c),
        send(targets, m.marks.at[p], (m.start_sems.at[1, 0], m.start_sems.at[1, 1]), partner, c),
    ]

    @pl.when(first)
    def _():
        up_column()
        down_column()

    for k in range(1, S):
        sems = pair(m.gain_sems, k)
        send(gain.at[:, cut_of(2 * section(k) + p)], m.gains.at[c], sems, pos, section(k))
    local(gain.at[:, cut_of(q)], m.gains.at[c], m.gain_sems.at[1, 0])

    id_hot = (lax.broadcasted_iota(i32, (R, R), 0) == ids[...] - pos * R).astype(bf16)
    taken = (lax.broadcasted_iota(i32, (V, R), 0) == sampled[0:1]).astype(bf16)
    for n in range(2):
        loads[2 * n].wait()
        loads[2 * n + 1].wait()
        start = (contract_first(id_hot, m.rep[n]) + contract_first(taken, m.tab[n])).astype(bf16)
        mine_rows = pl.ds(pl.multiple_of(p * R, R), R)
        if n == 0:
            m.away[...] = start
            sems = (m.start_sems.at[2, 0], m.start_sems.at[2, 1])
            moved = send(m.away, states.at[0, mine_rows], sems, partner, c)
        else:
            states[0, mine_rows] = start

    chip, row = lax.div(c * GS, R), pl.multiple_of(lax.rem(c * GS, R), GS)

    def count():
        m.marks[p] = targets[...]
        m.picks[p] = sampled[...]
        land(extra)
        picks, marks = m.picks[chip], m.marks[chip]
        actions = lax.broadcasted_iota(i32, (V, R), 0)
        counts, hots = jnp.zeros((V, R), f32), jnp.zeros((V, R), f32)
        for k in range(d.samples):
            hit = jnp.where(picks[k : k + 1] == actions, 1.0, 0.0)
            counts += hit
            hots += jnp.where(marks == k, hit, 0.0)
        m.counts[...] = counts.T
        m.hots[...] = hots.T

    fans = {}
    relayed = I == 4

    def block(kind, layer, at, half=None):
        if kind == 0:
            if half is None:
                return ups.at[layer, at]
            return ups.at[layer, at, pl.ds(half * (d.up_held // 2), d.up_held // 2)]
        if half is None:
            return downs.at[layer, :, at]
        return downs.at[layer, pl.ds(half * (O // 2), O // 2), at]

    def blocks(kind, layer, n):
        return ups.at[layer, pl.ds(0, n)] if kind == 0 else downs.at[layer, :, pl.ds(0, n)]

    def fan(kind, layer):
        if kind == 0:
            arrive(ups.at[layer, j], m.col_up.at[1, layer])
        else:
            arrive(downs.at[layer, :, j], m.col_down.at[layer])
        going, coming = m.square_send.at[kind, layer], m.square_recv.at[kind, layer]
        made = fans[kind, layer] = {}
        if relayed:
            for k, half, n in ((1, 0, 0), (2, 1, 1), (1, 1, 2), (2, 0, 2)):
                view = block(kind, layer, j, half)
                to = z * I + flip(j, k)
                made[n] = send(view, view, (going, coming.at[n]), to, c, False)
        else:
            view = block(kind, layer, j)
            for k in range(1, I):
                to = z * I + square(k)
                made[k] = send(view, view, (going, coming.at[k - 1]), to, c, False)
        settle(blocks(kind, layer, I - 1), going)

    def relay(kind, layer):
        if relayed:
            made = fans[kind, layer]
            going, coming = m.square_send.at[kind, layer], m.square_recv.at[kind, layer]
            for k, half in ((1, 0), (2, 1)):
                land([made[half]])
                view = block(kind, layer, flip(j, k), half)
                send(view, view, (going, coming.at[2]), z * I + flip(j, 3 - k), c, False)

    def land_fan(kind, layer):
        if relayed:
            arrive(blocks(kind, layer, 2), m.square_recv.at[kind, layer, 2])
        else:
            land(fans[kind, layer])

    def land(made):
        for copy in made.values() if isinstance(made, dict) else made:
            copy.wait_recv()

    def tally(e, slot, stat):
        for k in range(S):
            m.stat_cuts[slot, k] = spread(GS, stat[k * GS : (k + 1) * GS], 0)
        rows = [
            send(
                m.stat_cuts.at[slot, section(k)],
                m.stat_got.at[slot, k],
                pair(m.tallies, slot, 0, k - 1),
                pos,
                section(k),
            )
            for k in range(1, S)
        ]

        def finish():
            land(rows)
            row = m.stat_cuts[slot, c]
            for k in range(1, S):
                row += m.stat_got[slot, k]
            m.stat_swap[slot, 0] = row
            swap = m.stat_swap.at[slot]
            over = send(swap.at[0], swap.at[1], pair(m.tallies, slot, 1, 0), partner, c)

            def end():
                land([over])
                return spread(GS, row + m.stat_swap[slot, 1], 1)

            return end

        return finish

    def trade(e, partial, cuts, got, swap):
        m_acc = m.acc
        span = partial.shape[1]
        split = partial.reshape(S, GS, span)
        m_acc[:, :, :span] = split
        cuts[...] = split.astype(cuts.dtype)
        sent = [
            send(cuts.at[section(k)], got.at[k], pair(m.trade, e, 0, k - 1), pos, section(k))
            for k in range(1, S)
        ]

        def finish():
            land(sent)
            total = m_acc[c, :, :span]
            for k in range(1, S):
                total += got[k].astype(f32)
            swap[0] = total.astype(swap.dtype)
            over = send(swap.at[0], swap.at[1], pair(m.trade, e, 1, 0), partner, c)

            def end():
                land([over])
                return total + swap[1].astype(f32)

            return end

        return finish

    def gather(e, held):
        return [
            send(held.at[c], held.at[c], pair(m.trade, e, 2, k - 1), pos, section(k))
            for k in range(1, S)
        ]

    fan(0, 0)
    count()
    relay(0, 0)
    fan(1, 0)
    pl.when(later)(up_column)
    moved.wait_recv()
    arrive(m.gains.at[c], m.gain_sems.at[1, 0])
    for k in range(1, S):
        giver = lax.rem(c + S - k, S)
        arrive(m.gains.at[giver], m.gain_sems.at[1, k])

    def lend(layer):
        if d.factored:
            own = pl.ds(pl.multiple_of(j * d.up_held, 128), d.up_held)
            m.others[layer, j] = ready[layer, :, own]
            for k in (1, 2, 3):
                send(
                    ready.at[layer, :, pl.ds(pl.multiple_of(flip(j, k) * d.up_held, 128), d.up_held)],
                    m.others.at[layer, j],
                    pair(m.other_sems, layer),
                    z * I + flip(j, k),
                    c,
                    False,
                )
            settle(m.others.at[layer, pl.ds(0, I - 1)], m.other_sems.at[0, layer])

    def ups_of(layer):
        return ups[layer].reshape(W, FF)

    def downs_of(layer):
        return downs[layer].reshape(FF, W)

    for layer in range(S):
        wide = states[layer].astype(f32)
        ready[layer] = (wide * m.gains[layer]).astype(bf16)
        counted = tally(layer, layer, jnp.sum(wide * wide, -1, keepdims=True))
        land_fan(0, layer)
        partial = dot(ready[layer], ups_of(layer))
        middle = trade(layer, partial, m.cuts.at[layer], m.got.at[layer], m.swap.at[layer])
        counted = counted()
        if layer == 0:
            pl.when(later)(down_column)
        relay(1, layer)
        if layer + 1 == S:
            for held_layer in range(S):
                lend(held_layer)
        end = middle()
        if layer + 1 < S:
            fan(0, layer + 1)
        factor = lax.rsqrt(counted() / d.width + epsilon)
        value = end() * factor
        m.uppers[layer] = value
        m.recips[layer] = factor
        held = m.actives.at[layer]
        held[c] = (value * jax.nn.sigmoid(value)).astype(bf16)
        moving = gather(layer, held)
        if layer + 1 < S:
            relay(0, layer + 1)
            fan(1, layer + 1)
        land_fan(1, layer)
        land(moving)
        states[layer + 1] = (
            states[layer].astype(f32) + dot(m.actives[layer].reshape(G, FF), downs_of(layer))
        ).astype(bf16)

    part = contract_last(states[S], m.tab[1])
    total = trade(S, part, m.score_cuts, m.score_got, m.score_swap)()()
    bent = jnp.tanh(total / scale / logit_cap)
    logits = logit_cap * bent
    counts, hots = m.counts[pl.ds(row, GS)], m.hots[pl.ds(row, GS)]
    weighted = counts * jnp.exp(logits)
    summed = jnp.sum(weighted, -1, keepdims=True)
    d_scores = (weighted / summed - hots) / ROWS_DEV * (1.0 - bent * bent) / scale
    m.d_all[c] = d_scores.astype(bf16)
    moving = gather(S, m.d_all)
    cross = jnp.log(summed) - jnp.sum(logits * hots, -1, keepdims=True)
    counted = jnp.where(p == 0, 1.0 / ROWS_DEV, 0.0)
    loss_here = jnp.broadcast_to(jnp.sum(cross, 0, keepdims=True) * counted, (1, 128))
    land(moving)
    m.grad[...] = dot(m.d_all[...].reshape(G, V), m.tab[1]).astype(bf16)

    folds = {}

    def fold(kind, layer, source, dest):
        folds[kind, layer] = [
            send(source(square(k)), dest.at[layer, k - 1], pair(m.fold, kind, layer, k - 1), z * I + square(k), c)
            for k in range(1, I)
        ]

    def fold_down(layer):
        if not d.factored:
            fold(1, layer, lambda at: m.g_down.at[layer, :, at], m.down_in)
            return
        made = folds[1, layer] = {}
        for n, k, at, half in ((1, 1, 3, 0), (3, 2, 3, 1), (0, 1, 1, 0), (2, 2, 2, 1)):
            source = m.g_down.at[layer, pl.ds(half * (O // 2), O // 2), flip(j, at)]
            sems = (m.half_send.at[layer], m.half_recv.at[layer, {1: 0, 3: 1}.get(n, 2)])
            made[n] = send(source, m.down_in.at[layer, n], sems, z * I + flip(j, k), c, False)

    def refold_down(layer):
        if not d.factored:
            return
        made = folds[1, layer]
        for n, k, half in ((1, 2, 0), (3, 1, 1)):
            land([made[n]])
            own = m.g_down[layer, half * (O // 2) : (half + 1) * (O // 2), flip(j, k)]
            into = m.down_part.at[layer, half]
            into[...] = (own.astype(f32) + m.down_in[layer, n].astype(f32)).astype(bf16)
            sems = (m.half_send.at[layer], m.half_recv.at[layer, 2])
            send(into, m.down_in.at[layer, 4 + half], sems, z * I + flip(j, k), c, False)
        settle(m.down_in.at[layer], m.half_send.at[layer])

    def down_total(layer):
        if not d.factored:
            land(folds[1, layer])
            value = m.g_down[layer, :, j].astype(f32)
            for k in range(1, I):
                value += m.down_in[layer, k - 1].astype(f32)
            m.down_sum[layer] = value.astype(bf16)
            return
        arrive(m.down_in.at[layer, pl.ds(0, 4)], m.half_recv.at[layer, 2])
        for half in range(2):
            rows = pl.ds(half * (O // 2), O // 2)
            value = m.g_down[layer, rows, j].astype(f32)
            for n in (2 * half, 4 + half):
                value += m.down_in[layer, n].astype(f32)
            m.down_sum[layer, rows] = value.astype(bf16)

    def share(layer):
        held = m.d_uppers.at[layer, j, c]
        folds[0, layer] = [
            (k, send(held, held, (m.upper_send.at[layer], m.upper_recv.at[layer, k - 1]), z * I + flip(j, k), c, False))
            for k in (1, 2, 3)
        ]
        settle(m.d_uppers.at[layer, pl.ds(0, I - 1), 0], m.upper_send.at[layer])

    def up_total(layer):
        if not d.factored:
            land(folds[0, layer])
            value = m.g_up[layer, j].astype(f32)
            for k in range(1, I):
                value += m.up_in[layer, k - 1].astype(f32)
            m.up_sum[layer] = value.astype(bf16)
            return
        for k, made in folds[0, layer]:
            land([made])
            held = m.d_uppers.at[layer, flip(j, k), c]
            for b in range(1, S):
                send(held, held, pair(m.share_sems, layer), pos, section(b), False)
        passed = m.d_uppers.at[layer, pl.ds(0, I - 1), pl.ds(0, S - 1)]
        settle(passed, m.share_sems.at[0, layer])
        arrive(m.others.at[layer, pl.ds(0, I - 1)], m.other_sems.at[1, layer])
        arrive(passed, m.share_sems.at[1, layer])
        value = contract_first(
            m.others[layer].reshape(I * G, d.up_held), m.d_uppers[layer].reshape(I * G, FF)
        )
        m.up_sum[layer] = value.astype(bf16)

    home = q * I + j

    def end_down(layer):
        down_total(layer)
        for a in range(O):
            there = lax.rem(z + a, O)
            source, dest = m.down_sum.at[layer, there], m.down_end.at[zh, q]
            sems = (m.end_down.at[0 if a else 1, layer], m.end_down_recv.at[0])
            if a:
                send(source, dest, sems, column(a), layer, False)
            else:
                deliver(c == layer, source, dest, sems, pos, layer)
        settle(m.down_end.at[0, pl.ds(0, O - 1)], m.end_down.at[0, layer])

    def end_small(layer):
        arrive(m.small_in.at[layer], m.small_fold.at[1, layer])
        value = m.small[layer]
        for k in range(1, I):
            value += m.small_in[layer, k - 1]
        m.small_sum[layer] = value
        for a in range(O):
            source, dest = m.small_sum.at[layer], m.small_end.at[zh, q]
            sems = (m.end_small.at[0 if a else 1, layer], m.end_small_recv.at[0])
            if a:
                send(source, dest, sems, column(a), layer, False)
            else:
                deliver(c == layer, source, dest, sems, pos, layer)
        settle(m.small_end.at[0, pl.ds(0, O - 1)], m.end_small.at[0, layer])

    def end_up(layer):
        up_total(layer)
        sems = (m.end_up.at[layer], m.end_up_recv.at[0])
        mine = jnp.logical_and(c == zh, c == layer)
        deliver(mine, m.up_sum.at[layer], m.up_end.at[zh], sems, home, layer)

    for layer in reversed(range(S)):
        e = S + 1 + layer
        slot = S + layer
        grad = m.grad[...]
        part = contract_last(grad, downs_of(layer))
        middle = trade(e, part, m.cuts.at[slot], m.got.at[slot], m.swap.at[slot])
        if layer + 1 < S:
            refold_down(layer + 1)
        end = middle()
        actives = m.actives[layer].reshape(G, FF)
        m.g_down[layer] = contract_first(actives, grad).astype(bf16).reshape(O, I, d.ff_held, W)
        fold_down(layer)
        if not layer:
            settled = pending[:]
            pending.clear()
        total = end()
        value, factor = m.uppers[layer], m.recips[layer]
        sigm = jax.nn.sigmoid(value)
        d_upper = (total * sigm * (1.0 + value * (1.0 - sigm)) * factor).astype(bf16)
        held = m.d_uppers.at[layer, j if d.factored else 0]
        held[c] = d_upper
        moving = gather(e, held)
        if layer and d.factored:
            share(layer)
        if layer:
            pull = jnp.sum(d_upper.astype(f32) * value, -1, keepdims=True) * factor / d.width
            m.pulls[layer, c] = spread(GS, pull, 0)
            moving += [
                send(
                    m.pulls.at[layer, c],
                    m.pulls.at[layer, c],
                    pair(m.pull_sems, layer, k - 1),
                    pos,
                    section(k),
                )
                for k in range(1, S)
            ]
        land(moving)
        d_all = held[...].reshape(G, FF)
        wide = states[layer].astype(f32)
        d_normed = contract_last(d_all, ups_of(layer))
        m.small[layer, :, :W] = jnp.sum(d_normed * wide, 0, keepdims=True)
        m.small[layer, :, W:] = loss_here
        if layer:
            columns = jnp.concatenate([spread(GS, m.pulls[layer, k], 1) for k in range(S)], 0)
            m.grad[...] = (
                grad.astype(f32) + d_normed * m.gains[layer] - wide * columns
            ).astype(bf16)
        for k in range(1, I):
            sems = pair(m.small_fold, layer)
            send(m.small.at[layer], m.small_in.at[layer, k - 1], sems, z * I + square(k), c, False)
        settle(m.small_in.at[layer], m.small_fold.at[0, layer])
        if not d.factored:
            m.g_up[layer] = contract_first(ready[layer], d_all).astype(bf16).reshape(I, d.up_held, FF)
            fold(0, layer, lambda at: m.g_up.at[layer, at], m.up_in)
        if layer + 1 < S:
            end_up(layer + 1)
            end_small(layer + 1)
            end_down(layer + 1)
    refold_down(0)
    if d.factored:
        share(0)
    drain_columns()
    for finish in settled:
        finish()
    end_down(0)
    end_small(0)
    end_up(0)
    arrive(m.small_end, m.end_small_recv.at[0])
    arrive(m.down_end, m.end_down_recv.at[0])
    for finish in pending:
        finish()
    arrive(m.up_end, m.end_up_recv.at[0])


def sum_kernel(d, up_end, down_end, small_end, grad_up, grad_down, grad_gain, loss):
    W = d.cut

    def total(pieces):
        value = pieces[0].astype(f32)
        for piece in pieces[1:]:
            value += piece.astype(f32)
        return value

    groups = range(d.sections)
    lost = []
    grad_up[...] = total([up_end[h] for h in groups])
    for cut in range(d.outer):
        at = slice(cut * W, (cut + 1) * W)
        grad_down[:, at] = total([down_end[h, cut] for h in groups])
        grad_gain[:, at] = total([small_end[h, cut, :, :W] for h in groups])
        lost += [small_end[h, cut, :, W:] for h in groups]
    loss[0, 0] = total(lost)[0, 0]


def on_device(replay, state_ids, sampled, targets, action_table, norm_gain, w_up, w_down):
    held, width = replay.shape
    d = Dims(
        lax.axis_size(SECTION),
        lax.axis_size(DP),
        held,
        width,
        w_up.shape[2],
        action_table.shape[0],
        sampled.shape[1],
        w_up.shape[1],
        w_down.shape[1],
    )
    scratch = scratch_of(d)
    vmem = pl.BlockSpec(memory_space=pltpu.VMEM)
    hbm = pl.BlockSpec(memory_space=pltpu.HBM)
    ends = (
        jax.ShapeDtypeStruct((d.sections, d.up_held, d.ff), bf16),
        jax.ShapeDtypeStruct((d.sections, d.outer, d.ff_held, d.cut), bf16),
        jax.ShapeDtypeStruct((d.sections, d.outer, 1, d.cut + 128), f32),
    )
    parts = pl.pallas_call(
        functools.partial(step_kernel, d, tuple(scratch)),
        out_shape=ends,
        in_specs=[hbm] * 8,
        out_specs=[vmem] * 3,
        scratch_shapes=list(scratch.values()),
        compiler_params=pltpu.CompilerParams(
            collective_id=0, has_side_effects=True, vmem_limit_bytes=48 * 1024 * 1024
        ),
    )(
        *(
            pltpu.with_memory_space_constraint(x, pltpu.HBM)
            for x in (
                replay,
                action_table,
                state_ids[None, :],
                sampled.T,
                targets[None, :],
                norm_gain,
                w_up[0],
                w_down[0],
            )
        )
    )
    outs = ((d.up_held, d.ff), (d.ff_held, width), (1, width), (1, 1))
    grad_up, grad_down, grad_gain, loss = pl.pallas_call(
        functools.partial(sum_kernel, d),
        out_shape=[jax.ShapeDtypeStruct(shape, f32) for shape in outs],
        in_specs=[vmem] * 3,
        out_specs=[vmem] * 3 + [pl.BlockSpec(memory_space=pltpu.SMEM)],
        compiler_params=pltpu.CompilerParams(vmem_limit_bytes=8 * 1024 * 1024),
    )(*parts)
    return (grad_up[None], grad_down[None], grad_gain, loss.reshape(()))


def solution(mesh):
    return jax.shard_map(
        on_device,
        mesh=mesh,
        in_specs=(
            P("dp", None),
            P("dp"),
            P("dp", None),
            P("dp"),
            P(),
            P("section", None),
            P("section", "dp", None),
            P("section", "dp", None),
        ),
        out_specs=(P("section", "dp", None), P("section", "dp", None), P("section", None), P()),
        check_vma=False,
    )
```
